32 devices in a mesh: row: 8 (over z, core), col: 4 (over y, x).
Axes of the slice: x: 2, y: 2, z: 4, core: 2. Of those that a mesh axis runs over, the one named last changes fastest.
Arguments:
- features: bfloat16 [8, 4, 1024, 602], P('row', 'col'), may hold values from -6 to 6
- local_mask: int32 [8, 4, 1024, 1024], P('row', 'col'), may hold values 0 or 1
- halo_mask: int32 [8, 4, 1024, 512], P('row', 'col'), may hold values 0 or 1
- boundary_index: int32 [8, 4, 512], P('row', 'col'), may hold values from 0 to 1023
- labels: int32 [8, 4, 1024], P('row', 'col'), may hold values from 0 to 40
- halo_first: bfloat16 [8, 4, 512, 602], P('row', 'col'), may hold values from -6 to 6
- halo_second: bfloat16 [8, 4, 512, 256], P('row', 'col'), may hold values from -4 to 4
- halo_third: bfloat16 [8, 4, 512, 256], P('row', 'col'), may hold values from -4 to 4
- return_second: bfloat16 [8, 4, 512, 256], P('row', 'col'), may hold values from -0.0059814453 to 0.0059814453
- return_third: bfloat16 [8, 4, 512, 256], P('row', 'col'), may hold values from -0.0059814453 to 0.0059814453
- weight_first: bfloat16 [602, 256], replicated, may hold values from -1 to 1
- weight_second: bfloat16 [256, 256], replicated, may hold values from -1.5 to 1.5
- weight_third: bfloat16 [256, 41], replicated, may hold values from -1.5 to 1.5
Outputs:
- grad_first: float32 [602, 256], replicated
- grad_second: float32 [256, 256], replicated
- grad_third: float32 [256, 41], replicated
- next_second: bfloat16 [8, 4, 512, 256], P('row', 'col')
- next_third: bfloat16 [8, 4, 512, 256], P('row', 'col')
- back_second: bfloat16 [8, 4, 512, 256], P('row', 'col')
- back_third: bfloat16 [8, 4, 512, 256], P('row', 'col')
The draws below stay inside these ranges and needn't reach their ends.
All inputs are finite; a program needn't handle non-finite values. No bound on the sum of `local_mask` or of `halo_mask` on one device may be relied on, other than what follows from the above.
Results may differ from the reference program's by a relative error of at most 0.007.
Values may be sent and summed in bfloat16 or wider, within the bound.
A program may use at most 64 MiB of HBM per device.

```python
import jax
import jax.numpy as jnp
from jax import lax

IN_DIM = 602
HIDDEN_SIZE = 256
CLASSES = 41
NODE_DEV = 1024
BOUND = 128
N_ROW = 8
N_COL = 4


def place_ends(drawn, key, smallest, top_value):
    index_at = [jax.random.randint(jax.random.fold_in(key, axis), (), 0, length) for axis, length in enumerate(drawn.shape)]
    widest = drawn.shape.index(max(drawn.shape))
    neighbour = index_at[:widest] + [(index_at[widest] + 1) % drawn.shape[widest]] + index_at[widest + 1:]
    return drawn.at[tuple(index_at)].set(smallest).at[tuple(neighbour)].set(top_value)


def level_of(rng, dims, cuts, smallest, top_value):
    def one(dim, blocks):
        steps = jax.random.uniform(jax.random.fold_in(jax.random.fold_in(rng, 6), dim), (blocks,), jnp.float32, smallest / len(cuts), top_value / len(cuts))
        return jnp.repeat(jnp.exp(steps), dims[dim] // blocks).reshape((-1,) + (1,) * (len(dims) - dim - 1))

    level = one(*cuts[0])
    for cut in cuts[1:]:
        level = level * one(*cut)
    return level


def bell_draw(rng, dims, scale, bound, cuts=(), held_as=jnp.bfloat16):
    entries = scale * jax.random.normal(rng, dims, jnp.float32)
    if cuts:
        entries = entries * level_of(rng, dims, cuts, -0.22, 0.18)
    return jnp.clip(entries, -bound, bound).astype(held_as)


def setup_inputs(seed: int = 0) -> dict:
    keys = jax.random.split(jax.random.key(seed), 14)
    return {
        "features": bell_draw(keys[0], (N_ROW, N_COL, NODE_DEV, IN_DIM), 1.0, 6.0, ((0, 8), (1, 4))),
        "local_mask": place_ends((jax.random.randint(keys[1], (N_ROW, N_COL, NODE_DEV, NODE_DEV), 0, NODE_DEV) < min(16, NODE_DEV // 4)).astype(jnp.int32), jax.random.fold_in(keys[1], 1), 0, 1),
        "halo_mask": place_ends((jax.random.randint(keys[2], (N_ROW, N_COL, NODE_DEV, 4 * BOUND), 0, BOUND) < min(2, BOUND // 4)).astype(jnp.int32), jax.random.fold_in(keys[2], 1), 0, 1),
        "boundary_index": place_ends(jax.random.randint(keys[3], (N_ROW, N_COL, 4 * BOUND), 0, NODE_DEV), jax.random.fold_in(keys[3], 1), 0, NODE_DEV - 1).astype(jnp.int32),
        "labels": place_ends(jax.random.randint(keys[4], (N_ROW, N_COL, NODE_DEV), 0, CLASSES), jax.random.fold_in(keys[4], 1), 0, CLASSES - 1).astype(jnp.int32),
        "halo_first": bell_draw(keys[5], (N_ROW, N_COL, 4 * BOUND, IN_DIM), 1.0, 6.0, ((0, 8), (1, 4))),
        "halo_second": bell_draw(keys[6], (N_ROW, N_COL, 4 * BOUND, HIDDEN_SIZE), 0.5, 4.0, ((0, 8), (1, 4))),
        "halo_third": bell_draw(keys[7], (N_ROW, N_COL, 4 * BOUND, HIDDEN_SIZE), 0.5, 4.0, ((0, 8), (1, 4))),
        "return_second": bell_draw(keys[8], (N_ROW, N_COL, 4 * BOUND, HIDDEN_SIZE), 0.001, 0.0059814453, ((0, 8), (1, 4))),
        "return_third": bell_draw(keys[9], (N_ROW, N_COL, 4 * BOUND, HIDDEN_SIZE), 0.001, 0.0059814453, ((0, 8), (1, 4))),
        "weight_first": bell_draw(keys[10], (IN_DIM, HIDDEN_SIZE), (IN_DIM // 16) ** -0.5, 1.0),
        "weight_second": bell_draw(keys[11], (HIDDEN_SIZE, HIDDEN_SIZE), (HIDDEN_SIZE // 16) ** -0.5, 1.5),
        "weight_third": bell_draw(keys[12], (HIDDEN_SIZE, CLASSES), (HIDDEN_SIZE // 16) ** -0.5, 1.5),
    }


def slope(pre):
    sigma = jax.nn.sigmoid(pre)
    return sigma * (1.0 + pre * (1.0 - sigma))


def spread(local_bf, halo_bf, inverse, values, remote):
    summed = jnp.dot(local_bf, values, preferred_element_type=jnp.float32)
    summed = summed + values.astype(jnp.float32)
    summed = summed + jnp.dot(halo_bf, remote, preferred_element_type=jnp.float32)
    return (summed * inverse).astype(jnp.bfloat16)


def retract(local_bf, halo_bf, inverse, upstream, weight, hits, returned):
    across = jnp.dot(upstream, weight.T, preferred_element_type=jnp.float32)
    scaled = (across * inverse).astype(jnp.bfloat16)
    carried = jnp.dot(local_bf.T, scaled, preferred_element_type=jnp.float32) + scaled.astype(jnp.float32)
    carried = carried + jnp.dot(hits, returned, preferred_element_type=jnp.float32)
    outgoing = jnp.dot(halo_bf.T, scaled, preferred_element_type=jnp.float32).astype(jnp.bfloat16)
    return carried, outgoing


def partition(features, local_mask, halo_mask, boundary_index, labels, halo_first, halo_second, halo_third,
              return_second, return_third, weight_first, weight_second, weight_third):
    local_bf = local_mask.astype(jnp.bfloat16)
    halo_bf = halo_mask.astype(jnp.bfloat16)
    degree = 1.0 + jnp.sum(local_mask, axis=1).astype(jnp.float32) + jnp.sum(halo_mask, axis=1).astype(jnp.float32)
    inverse = (1.0 / degree)[:, None]
    node_rows = features.shape[0]
    hits = (jnp.arange(node_rows, dtype=jnp.int32)[:, None] == boundary_index[None, :]).astype(jnp.bfloat16)
    mixed_one = spread(local_bf, halo_bf, inverse, features, halo_first)
    pre_one = jnp.dot(mixed_one, weight_first, preferred_element_type=jnp.float32)
    hidden_one = jax.nn.silu(pre_one).astype(jnp.bfloat16)
    mixed_two = spread(local_bf, halo_bf, inverse, hidden_one, halo_second)
    pre_two = jnp.dot(mixed_two, weight_second, preferred_element_type=jnp.float32)
    hidden_two = jax.nn.silu(pre_two).astype(jnp.bfloat16)
    mixed_three = spread(local_bf, halo_bf, inverse, hidden_two, halo_third)
    logits = jnp.dot(mixed_three, weight_third, preferred_element_type=jnp.float32)
    expo = jnp.exp(logits)
    probs = expo / jnp.sum(expo, axis=1, keepdims=True)
    target = (labels[:, None] == jnp.arange(logits.shape[1], dtype=jnp.int32)[None, :]).astype(jnp.float32)
    upstream_three = ((probs - target) / node_rows).astype(jnp.bfloat16)
    grad_three = jnp.dot(mixed_three.T, upstream_three, preferred_element_type=jnp.float32)
    carried_two, outgoing_three = retract(local_bf, halo_bf, inverse, upstream_three, weight_third, hits, return_third)
    upstream_two = (carried_two * slope(pre_two)).astype(jnp.bfloat16)
    grad_two = jnp.dot(mixed_two.T, upstream_two, preferred_element_type=jnp.float32)
    carried_one, outgoing_two = retract(local_bf, halo_bf, inverse, upstream_two, weight_second, hits, return_second)
    upstream_one = (carried_one * slope(pre_one)).astype(jnp.bfloat16)
    grad_one = jnp.dot(mixed_one.T, upstream_one, preferred_element_type=jnp.float32)
    sent_second = jnp.take(hidden_one, boundary_index, axis=0)
    sent_third = jnp.take(hidden_two, boundary_index, axis=0)
    return grad_one, grad_two, grad_three, sent_second, sent_third, outgoing_two, outgoing_three


def route(sent):
    parted = sent.reshape((N_ROW, N_COL, 4, BOUND, sent.shape[-1]))
    blank_row = jnp.zeros_like(parted[:1, :, 0])
    blank_col = jnp.zeros_like(parted[:, :1, 0])
    from_above = jnp.concatenate([blank_row, parted[:-1, :, 1]], axis=0)
    from_below = jnp.concatenate([parted[1:, :, 0], blank_row], axis=0)
    from_left = jnp.concatenate([blank_col, parted[:, :-1, 3]], axis=1)
    from_right = jnp.concatenate([parted[:, 1:, 2], blank_col], axis=1)
    return jnp.stack([from_above, from_below, from_left, from_right], axis=2).reshape(sent.shape)


def reference(features, local_mask, halo_mask, boundary_index, labels, halo_first, halo_second, halo_third,
              return_second, return_third, weight_first, weight_second, weight_third):
    partitions = N_ROW * N_COL

    def flatten(array):
        return array.reshape((partitions,) + array.shape[2:])

    def advance(totals, pieces):
        result = partition(*pieces, weight_first, weight_second, weight_third)
        return (totals[0] + result[0], totals[1] + result[1], totals[2] + result[2]), result[3:]

    start = (jnp.zeros(weight_first.shape, jnp.float32), jnp.zeros(weight_second.shape, jnp.float32),
             jnp.zeros(weight_third.shape, jnp.float32))
    inputs = tuple(flatten(array) for array in (features, local_mask, halo_mask, boundary_index, labels, halo_first,
                                                halo_second, halo_third, return_second, return_third))
    sums, sends = lax.scan(advance, start, inputs)
    shaped = [route(piece.reshape((N_ROW, N_COL) + piece.shape[1:])) for piece in sends]
    return sums[0], sums[1], sums[2], shaped[0], shaped[1], shaped[2], shaped[3]
```

```python
import functools

import jax
import jax.numpy as jnp
from jax import lax
from jax.experimental import pallas as pl
from jax.experimental.pallas import tpu as pltpu
from jax.sharding import PartitionSpec as P

MESH = pl.DeviceIdType.MESH
BF = jnp.bfloat16
F32 = jnp.float32


def up_to(value, step):
    return -(-value // step) * step


def dot(a, b, dims=((1,), (0,))):
    return lax.dot_general(a, b, (dims, ((), ())), preferred_element_type=F32)


def slope(pre):
    sigma = jax.nn.sigmoid(pre)
    return sigma * (1.0 + pre * (1.0 - sigma))


class Plan:
    def __init__(self, mesh, hidden):
        self.n_row, self.n_col = mesh.shape["row"], mesh.shape["col"]
        self.pair = 2 if self.n_row % 2 == 0 else 1
        self.deep = self.n_row // self.pair
        self.chips = self.deep * self.n_col
        self.lanes = hidden // self.pair
        deep = sorted(range(self.deep), key=lambda d: -min(d, self.deep - d))
        cols = sorted(range(self.n_col), key=lambda d: -min(d, self.n_col - d))
        self.ways = [(dz, dc) for dz in deep for dc in cols if dz or dc]

    def place(self):
        self.r, self.c = lax.axis_index("row"), lax.axis_index("col")
        self.core, self.z = self.r % self.pair, self.r // self.pair
        self.mate = self.r + 1 - 2 * self.core
        self.chip = self.z * self.n_col + self.c

    def peer(self, way, sign=1):
        z = (self.z + sign * way[0] + self.deep) % self.deep
        c = (self.c + sign * way[1] + self.n_col) % self.n_col
        return z * self.n_col + c, (z * self.pair + self.core, c)

    def greet(self):
        barrier = pltpu.get_barrier_semaphore()

        def hello(device):
            pl.semaphore_signal(barrier, inc=1, device_id=device, device_id_type=MESH)

        count = 0
        if self.pair == 2:
            hello((self.mate, self.c))
            count += 1
        for way in self.ways:
            hello(self.peer(way)[1])
            count += 1
        for step, there in self.far_rows():
            @pl.when(there)
            def _():
                hello((self.r + step, self.c))
        for _, there in self.far_rows():
            count = count + jnp.where(there, 1, 0)
        pl.semaphore_wait(barrier, count)

    def far_rows(self):
        if self.pair == 2:
            return ((-1, jnp.logical_and(self.core == 0, self.r > 0)),
                    (1, jnp.logical_and(self.core == 1, self.r < self.n_row - 1)))
        return ()

    def edges(self):
        r, c = self.r, self.c
        return (((r - 1, c), 1, r > 0), ((r + 1, c), 0, r < self.n_row - 1),
                ((r, c - 1), 3, c > 0), ((r, c + 1), 2, c < self.n_col - 1))


def halo_copy(plan, k, src, dst, send, recv, way):
    bound = src.shape[0] // 4
    device, slot, there = plan.edges()[k]
    copy = pltpu.make_async_remote_copy(
        src_ref=src.at[pl.ds(k * bound, bound)], dst_ref=dst.at[pl.ds(slot * bound, bound)],
        send_sem=send.at[way, k], recv_sem=recv.at[way, slot], device_id=device, device_id_type=MESH)
    return copy, slot, there


def halo_start(plan, src, dst, send, recv, way):
    bound = src.shape[0] // 4
    for k in range(4):
        copy, _, there = halo_copy(plan, k, src, dst, send, recv, way)

        @pl.when(there)
        def _():
            copy.start()

        @pl.when(jnp.logical_not(there))
        def _():
            dst[pl.ds(k * bound, bound), :] = jnp.zeros((bound, dst.shape[1]), dst.dtype)


def halo_finish(plan, src, dst, send, recv, way):
    bound = src.shape[0] // 4
    for k in range(4):
        copy, _, there = halo_copy(plan, k, src, dst, send, recv, way)
        arrival = pltpu.make_async_remote_copy(
            src_ref=src.at[pl.ds(k * bound, bound)], dst_ref=dst.at[pl.ds(k * bound, bound)],
            send_sem=send.at[way, k], recv_sem=recv.at[way, k], device_id=plan.edges()[k][0], device_id_type=MESH)

        @pl.when(there)
        def _():
            copy.wait_send()
            arrival.wait_recv()


class Summer:
    def __init__(self, plan, sizes, own, mine, got_pair, acc, got, whole, sems):
        self.plan, self.sizes, self.own, self.mine, self.got_pair = plan, sizes, own, mine, got_pair
        self.acc, self.got, self.whole, self.sems = acc, got, whole, sems

    def copy(self, src, dst, kind, d, device):
        return pltpu.make_async_remote_copy(
            src_ref=src, dst_ref=dst, send_sem=self.sems[2 * kind].at[d], recv_sem=self.sems[2 * kind + 1].at[d],
            device_id=device, device_id_type=MESH)

    def clear(self):
        self.own[...] = jnp.zeros_like(self.own)
        self.mine[...] = jnp.zeros_like(self.mine)

    def put(self, i, value):
        at, chunk = slabs(self.sizes, self.plan.chips)[i]
        for core in range(self.plan.pair):
            part = value[:, core * self.plan.lanes:(core + 1) * self.plan.lanes]
            for k in range(-(-value.shape[0] // chunk)):
                rows = part[k * chunk:(k + 1) * chunk]
                self.own[core, k, at:at + rows.shape[0], :] = rows
                self.mine[core, k, at:at + rows.shape[0], :] = rows.astype(BF)

    def pair_copy(self):
        return self.copy(self.mine.at[1 - self.plan.core], self.got_pair, 0, 0, (self.plan.mate, self.plan.c))

    def start_pair(self):
        if self.plan.pair == 2:
            self.pair_copy().start()

    def spread_copy(self, d):
        index, device = self.plan.peer(self.plan.ways[d])
        return self.copy(self.acc.at[index], self.got.at[d], 1, d, device)

    def start_spread(self):
        if self.plan.pair == 2:
            self.pair_copy().wait()
            self.acc[...] = (self.own[self.plan.core] + self.got_pair[...].astype(F32)).astype(BF)
        else:
            self.acc[...] = self.mine[0]
        for d in range(len(self.plan.ways)):
            self.spread_copy(d).start()

    def gather_copy(self, d):
        part = self.whole.at[self.plan.core, self.plan.chip]
        return self.copy(part, part, 2, d, self.plan.peer(self.plan.ways[d])[1])

    def back_copy(self, d, core):
        index = self.plan.chip if d == len(self.plan.ways) else self.plan.peer(self.plan.ways[d], -1)[0]
        part = self.whole.at[core, index]
        return self.copy(part, part, 3, d, (self.plan.mate, self.plan.c))

    def start_gather(self):
        plan = self.plan
        total = self.own[plan.core, plan.chip]
        if plan.pair == 2:
            total = total + self.got_pair[plan.chip].astype(F32)
        for d in range(len(plan.ways)):
            self.spread_copy(d).wait()
        for d in range(len(plan.ways)):
            total = total + self.got[d].astype(F32)
        self.whole[plan.core, plan.chip] = total.astype(BF)
        for d in range(len(plan.ways)):
            self.gather_copy(d).start()
        if plan.pair == 2:
            self.back_copy(len(plan.ways), plan.core).start()

    def start_back(self):
        plan = self.plan
        for d in reversed(range(len(plan.ways))):
            index = plan.peer(plan.ways[d], -1)[0]
            part = self.whole.at[plan.core, index]
            self.copy(part, part, 2, d, plan.peer(plan.ways[d], -1)[1]).wait_recv()
            if plan.pair == 2:
                self.back_copy(d, plan.core).start()

    def finish(self):
        plan = self.plan
        for d in range(len(plan.ways)):
            self.gather_copy(d).wait_send()
        if plan.pair == 2:
            for d in range(len(plan.ways) + 1):
                self.back_copy(d, plan.core).wait_send()
                self.back_copy(d, 1 - plan.core).wait_recv()


def slabs(sizes, chips):
    out, at = [], 0
    for size in sizes:
        chunk = up_to(-(-size // chips), 8)
        out.append((at, chunk))
        at += chunk
    return out


def slab_rows(sizes, chips):
    return sum(chunk for _, chunk in slabs(sizes, chips))


def summer_scratch(plan, sizes):
    rows, dma, n = slab_rows(sizes, plan.chips), pltpu.SemaphoreType.DMA, max(len(plan.ways), 1)
    full = (plan.chips, rows, plan.lanes)
    return [pltpu.VMEM((plan.pair,) + full, F32), pltpu.VMEM((plan.pair,) + full, BF), pltpu.VMEM(full, BF),
            pltpu.VMEM(full, BF), pltpu.VMEM((n, rows, plan.lanes), BF),
            dma((1,)), dma((1,)), dma((n,)), dma((n,)), dma((n,)), dma((n,)), dma((n + 1,)), dma((n + 1,))]


SUMMER_REFS = 13


NAMES = ("local", "halo", "features", "halo_first", "halo_second", "halo_third", "return_second", "return_third",
         "weight_first", "weight_second", "weight_third", "index_row", "labels")


def step_kernel(plan, tiles, early_sizes, late_sizes, *refs):
    count = len(NAMES)
    hbm = dict(zip(NAMES, refs[:count]))
    whole_early, whole_late, n2, n3, b2, b3 = refs[count:count + 6]
    held = dict(zip(NAMES, refs[count + 6:2 * count + 6]))
    (in_sem, local_bf, halo_bf, inverse, hits, hits_t, mixed_one, mixed_two, mixed_three, pre_one, pre_two, hidden_one,
     hidden_two, scaled, upstream, upstream_three, target_held, s2, s3, o2, o3, hsend, hrecv) = refs[2 * count + 6:2 * count + 29]
    rest = refs[2 * count + 29:]
    early, late = (Summer(plan, sizes, *part[:5], whole, part[5:]) for sizes, part, whole in (
        (early_sizes, rest[:SUMMER_REFS], whole_early), (late_sizes, rest[SUMMER_REFS:], whole_late)))
    nodes = held["local"].shape[0]
    tall = nodes // tiles
    tile = [pl.ds(t * tall, tall) for t in range(tiles)]
    plan.place()

    loads = {}
    for name in ("index_row", "features", "halo_first", "local", "halo") + NAMES[4:11] + ("labels",):
        if name in ("local", "halo"):
            for t in range(tiles):
                key = (name, t)
                loads[key] = pltpu.make_async_copy(hbm[name].at[tile[t]], held[name].at[tile[t]], in_sem.at[len(loads)])
        else:
            loads[name] = pltpu.make_async_copy(hbm[name], held[name], in_sem.at[len(loads)])
    order = ["index_row", "features", "halo_first"]
    for t in range(tiles):
        order += [("local", t), ("halo", t)]
    order += [name for name in loads if name not in order]
    for key in order:
        loads[key].start()

    plan.greet()
    early.clear()
    late.clear()

    loads["index_row"].wait()
    slots = hits.shape[1]
    hits[...] = jnp.where(lax.broadcasted_iota(jnp.int32, (nodes, slots), 0) == held["index_row"][...], 1.0, 0.0).astype(BF)
    hits_t[...] = hits[...].T
    loads["labels"].wait()
    wide = target_held.shape[1]
    target_held[...] = jnp.where(lax.broadcasted_iota(jnp.int32, (wide, nodes), 0) == held["labels"][...], 1.0, 0.0).T
    loads["features"].wait()
    loads["halo_first"].wait()

    def spread(t, values, remote, out, dims=((1,), (0,))):
        total = dot(local_bf[tile[t], :], values[...], dims) + dot(halo_bf[tile[t], :], remote[...], dims)
        out[tile[t], :] = (total * inverse[tile[t], :]).astype(BF)

    for t in range(tiles):
        loads[("local", t)].wait()
        loads[("halo", t)].wait()
        near, far = held["local"][tile[t], :].astype(F32), held["halo"][tile[t], :].astype(F32)
        here = lax.broadcasted_iota(jnp.int32, near.shape, 0) + t * tall == lax.broadcasted_iota(jnp.int32, near.shape, 1)
        local_bf[tile[t], :] = jnp.where(here, near + 1.0, near).astype(BF)
        halo_bf[tile[t], :] = far.astype(BF)
        inverse[tile[t], :] = 1.0 / (1.0 + jnp.sum(near, axis=1, keepdims=True) + jnp.sum(far, axis=1, keepdims=True))
        spread(t, held["features"], held["halo_first"], mixed_one, ((1,), (1,)))
        if t == 0:
            for name in NAMES[4:11]:
                loads[name].wait()
        pre = dot(mixed_one[tile[t], :], held["weight_first"][...])
        pre_one[tile[t], :] = pre
        hidden_one[tile[t], :] = (pre * jax.nn.sigmoid(pre)).astype(BF)
    s2[...] = dot(hits_t[...], hidden_one[...]).astype(BF)
    halo_start(plan, s2, n2, hsend, hrecv, 0)
    for t in range(tiles):
        spread(t, hidden_one, held["halo_second"], mixed_two)
        pre = dot(mixed_two[tile[t], :], held["weight_second"][...])
        pre_two[tile[t], :] = pre
        hidden_two[tile[t], :] = (pre * jax.nn.sigmoid(pre)).astype(BF)
    s3[...] = dot(hits_t[...], hidden_two[...]).astype(BF)
    halo_start(plan, s3, n3, hsend, hrecv, 1)
    for t in range(tiles):
        spread(t, hidden_two, held["halo_third"], mixed_three)
        logits = dot(mixed_three[tile[t], :], held["weight_third"][...], ((1,), (1,)))
        expo = jnp.exp(logits)
        probs = expo / jnp.sum(expo, axis=1, keepdims=True)
        target = target_held[tile[t], :logits.shape[1]]
        up = ((probs - target) / nodes).astype(BF)
        upstream_three[tile[t], :] = up
        scaled[tile[t], :] = (dot(up, held["weight_third"][...]) * inverse[tile[t], :]).astype(BF)
    turn = ((0,), (0,))

    def carry(t, returned):
        return dot(local_bf[:, tile[t]], scaled[...], turn) + dot(hits[tile[t], :], returned[...])

    for t in range(tiles):
        upstream[tile[t], :] = (carry(t, held["return_third"]) * slope(pre_two[tile[t], :])).astype(BF)
    early.put(0, dot(mixed_two[...], upstream[...], turn))
    early.put(1, dot(upstream_three[...], mixed_three[...], turn))
    early.start_pair()
    o3[...] = dot(halo_bf[...], scaled[...], turn).astype(BF)
    halo_start(plan, o3, b3, hsend, hrecv, 2)
    for t in range(tiles):
        across = dot(upstream[tile[t], :], held["weight_second"][...], ((1,), (1,)))
        scaled[tile[t], :] = (across * inverse[tile[t], :]).astype(BF)
    early.start_spread()
    for t in range(tiles):
        upstream[tile[t], :] = (carry(t, held["return_second"]) * slope(pre_one[tile[t], :])).astype(BF)
    late.put(0, dot(mixed_one[...], upstream[...], turn))
    late.start_pair()
    o2[...] = dot(halo_bf[...], scaled[...], turn).astype(BF)
    late.start_spread()
    early.start_gather()
    halo_start(plan, o2, b2, hsend, hrecv, 3)
    late.start_gather()
    early.start_back()
    late.start_back()
    early.finish()
    late.finish()
    for way, (src, dst) in enumerate(((s2, n2), (s3, n3), (o3, b3), (o2, b2))):
        halo_finish(plan, src, dst, hsend, hrecv, way)


def finish_kernel(plan, early_sizes, late_sizes, whole_early, whole_late, n2, n3, b2, b3, g1, g2, g3, m2, m3, a2, a3, h1, h2, h3, sem):
    copies = [pltpu.make_async_copy(src, dst, sem.at[i]) for i, (src, dst) in enumerate(((n2, m2), (n3, m3), (b2, a2), (b3, a3)))]
    for copy in copies:
        copy.start()
    for i, (ref, out, whole, sizes, part) in enumerate((
            (h1, g1, whole_late, late_sizes, 0), (h2, g2, whole_early, early_sizes, 0), (h3, g3, whole_early, early_sizes, 1))):
        at, chunk = slabs(sizes, plan.chips)[part]
        for core in range(plan.pair):
            for k in range(-(-ref.shape[0] // chunk)):
                rows = min(chunk, ref.shape[0] - k * chunk)
                ref[k * chunk:k * chunk + rows, core * plan.lanes:(core + 1) * plan.lanes] = whole[core, k, at:at + rows, :].astype(F32)
        copies.append(pltpu.make_async_copy(ref, out, sem.at[4 + i]))
        copies[-1].start()
    for copy in copies:
        copy.wait()


def per_device(mesh, features, local_mask, halo_mask, boundary_index, labels, halo_first, halo_second, halo_third,
               return_second, return_third, weight_first, weight_second, weight_third):
    features, local_mask, halo_mask = features[0, 0], local_mask[0, 0], halo_mask[0, 0]
    index, labels = boundary_index[0, 0], labels[0, 0]
    halo_first, halo_second, halo_third = halo_first[0, 0], halo_second[0, 0], halo_third[0, 0]
    return_second, return_third = return_second[0, 0], return_third[0, 0]
    nodes, width = features.shape
    slots, hidden, classes = index.shape[0], weight_first.shape[1], weight_third.shape[1]
    plan = Plan(mesh, hidden)
    early_sizes, late_sizes = (weight_second.shape[0], classes), (width,)
    tiles = 4 if nodes % 512 == 0 else 1
    values = (local_mask, halo_mask, features.T, halo_first.T, halo_second, halo_third, return_second, return_third,
              weight_first, weight_second, weight_third.T, index[None, :], labels[None, :])
    vmem, anywhere = pl.BlockSpec(memory_space=pltpu.VMEM), pl.BlockSpec(memory_space=pl.ANY)
    dma = pltpu.SemaphoreType.DMA
    block = jax.ShapeDtypeStruct((slots, hidden), BF)
    done = pl.pallas_call(
        functools.partial(step_kernel, plan, tiles, early_sizes, late_sizes),
        out_shape=tuple(jax.ShapeDtypeStruct((plan.pair, plan.chips, slab_rows(sizes, plan.chips), plan.lanes), BF)
                        for sizes in (early_sizes, late_sizes)) + (block,) * 4,
        in_specs=[anywhere] * len(values), out_specs=(vmem,) * 6,
        scratch_shapes=[pltpu.VMEM(v.shape, v.dtype) for v in values] + [
            dma((len(values) + 2 * tiles,)), pltpu.VMEM((nodes, nodes), BF), pltpu.VMEM((nodes, slots), BF), pltpu.VMEM((nodes, 1), F32),
            pltpu.VMEM((nodes, slots), BF), pltpu.VMEM((slots, nodes), BF),
            pltpu.VMEM((nodes, width), BF), pltpu.VMEM((nodes, hidden), BF), pltpu.VMEM((nodes, hidden), BF),
            pltpu.VMEM((nodes, hidden), F32), pltpu.VMEM((nodes, hidden), F32),
            pltpu.VMEM((nodes, hidden), BF), pltpu.VMEM((nodes, hidden), BF), pltpu.VMEM((nodes, hidden), BF),
            pltpu.VMEM((nodes, hidden), BF), pltpu.VMEM((nodes, classes), BF),
            pltpu.VMEM((nodes, up_to(classes, 128)), F32)]
        + [pltpu.VMEM((slots, hidden), BF)] * 4 + [dma((4, 4)), dma((4, 4))]
        + summer_scratch(plan, early_sizes) + summer_scratch(plan, late_sizes),
        compiler_params=pltpu.CompilerParams(collective_id=0, has_side_effects=True),
        name="step",
    )(*values)
    grads = ((weight_first.shape, F32), (weight_second.shape, F32), (weight_third.shape[::-1], F32))
    out = pl.pallas_call(
        functools.partial(finish_kernel, plan, early_sizes, late_sizes),
        out_shape=tuple(jax.ShapeDtypeStruct(*g) for g in grads) + (block,) * 4,
        in_specs=[vmem] * 6, out_specs=(anywhere,) * 7,
        scratch_shapes=[pltpu.VMEM(*g) for g in grads] + [dma((7,))],
        name="finish",
    )(*done)
    return (out[0], out[1], out[2].T) + tuple(v[None, None] for v in out[3:])


def solution(mesh):
    wide, flat, copied = P("row", "col", None, None), P("row", "col", None), P()
    return jax.shard_map(
        functools.partial(per_device, mesh), mesh=mesh,
        in_specs=(wide, wide, wide, flat, flat, wide, wide, wide, wide, wide, copied, copied, copied),
        out_specs=(copied, copied, copied, wide, wide, wide, wide),
        check_vma=False,
    )
```

```python
import functools

import jax
import jax.numpy as jnp
from jax import lax
from jax.experimental import pallas as pl
from jax.experimental.pallas import tpu as pltpu
from jax.sharding import PartitionSpec as P

MESH = pl.DeviceIdType.MESH
BF = jnp.bfloat16
F32 = jnp.float32


def up_to(value, step):
    return -(-value // step) * step


def dot(a, b, dims=((1,), (0,))):
    return lax.dot_general(a, b, (dims, ((), ())), preferred_element_type=F32)


def slope(pre, sigma):
    return sigma * (1.0 + pre * (1.0 - sigma))


class Plan:
    def __init__(self, mesh, hidden):
        self.n_row, self.n_col = mesh.shape["row"], mesh.shape["col"]
        self.pair = 2 if self.n_row % 2 == 0 else 1
        self.deep = self.n_row // self.pair
        self.chips = self.deep * self.n_col
        self.lanes = hidden // self.pair
        deep = sorted(range(self.deep), key=lambda d: -min(d, self.deep - d))
        cols = sorted(range(self.n_col), key=lambda d: -min(d, self.n_col - d))
        self.ways = [(dz, dc) for dz in deep for dc in cols if dz or dc]

    def place(self):
        self.r, self.c = lax.axis_index("row"), lax.axis_index("col")
        self.core, self.z = self.r % self.pair, self.r // self.pair
        self.mate = self.r + 1 - 2 * self.core
        self.chip = self.z * self.n_col + self.c

    def peer(self, way, sign=1):
        z = (self.z + sign * way[0] + self.deep) % self.deep
        c = (self.c + sign * way[1] + self.n_col) % self.n_col
        return z * self.n_col + c, (z * self.pair + self.core, c)

    def greet(self):
        barrier = pltpu.get_barrier_semaphore()

        def hello(device):
            pl.semaphore_signal(barrier, inc=1, device_id=device, device_id_type=MESH)

        count = 0
        if self.pair == 2:
            hello((self.mate, self.c))
            count += 1
        for way in self.ways:
            hello(self.peer(way)[1])
            count += 1
        for step, there in self.far_rows():
            @pl.when(there)
            def _():
                hello((self.r + step, self.c))
        for _, there in self.far_rows():
            count = count + jnp.where(there, 1, 0)
        pl.semaphore_wait(barrier, count)

    def far_rows(self):
        if self.pair == 2:
            return ((-1, jnp.logical_and(self.core == 0, self.r > 0)),
                    (1, jnp.logical_and(self.core == 1, self.r < self.n_row - 1)))
        return ()

    def edges(self):
        r, c = self.r, self.c
        return (((r - 1, c), 1, r > 0), ((r + 1, c), 0, r < self.n_row - 1),
                ((r, c - 1), 3, c > 0), ((r, c + 1), 2, c < self.n_col - 1))


def halo_copy(plan, k, src, dst, send, recv, way):
    bound = src.shape[0] // 4
    device, slot, there = plan.edges()[k]
    copy = pltpu.make_async_remote_copy(
        src_ref=src.at[pl.ds(k * bound, bound)], dst_ref=dst.at[pl.ds(slot * bound, bound)],
        send_sem=send.at[way, k], recv_sem=recv.at[way, slot], device_id=device, device_id_type=MESH)
    return copy, slot, there


def halo_start(plan, src, dst, send, recv, way):
    bound = src.shape[0] // 4
    for k in range(4):
        copy, _, there = halo_copy(plan, k, src, dst, send, recv, way)

        @pl.when(there)
        def _():
            copy.start()


def halo_clear(plan, dsts):
    bound = dsts[0].shape[0] // 4
    for k in range(4):
        @pl.when(jnp.logical_not(plan.edges()[k][2]))
        def _():
            for dst in dsts:
                dst[pl.ds(k * bound, bound), :] = jnp.zeros((bound, dst.shape[1]), dst.dtype)


def halo_finish(plan, src, dst, send, recv, way):
    bound = src.shape[0] // 4
    for k in range(4):
        copy, _, there = halo_copy(plan, k, src, dst, send, recv, way)
        arrival = pltpu.make_async_remote_copy(
            src_ref=src.at[pl.ds(k * bound, bound)], dst_ref=dst.at[pl.ds(k * bound, bound)],
            send_sem=send.at[way, k], recv_sem=recv.at[way, k], device_id=plan.edges()[k][0], device_id_type=MESH)

        @pl.when(there)
        def _():
            copy.wait_send()
            arrival.wait_recv()


class Summer:
    def __init__(self, plan, sizes, own, mine, got_pair, acc, got, whole, sems):
        self.plan, self.sizes, self.own, self.mine, self.got_pair = plan, sizes, own, mine, got_pair
        self.acc, self.got, self.whole, self.sems = acc, got, whole, sems

    def copy(self, src, dst, kind, d, device):
        return pltpu.make_async_remote_copy(
            src_ref=src, dst_ref=dst, send_sem=self.sems[2 * kind].at[d], recv_sem=self.sems[2 * kind + 1].at[d],
            device_id=device, device_id_type=MESH)

    def clear(self):
        self.own[...] = jnp.zeros_like(self.own)
        self.mine[...] = jnp.zeros_like(self.mine)

    def put(self, i, value, row=0):
        at, chunk = slabs(self.sizes, self.plan.chips)[i]
        end = min(row + value.shape[0], self.sizes[i])
        for k in range(row // chunk, -(-end // chunk)):
            low, high = max(row, k * chunk), min(end, (k + 1) * chunk)
            for core in range(self.plan.pair):
                part = value[low - row:high - row, core * self.plan.lanes:(core + 1) * self.plan.lanes]
                place = slice(at + low - k * chunk, at + high - k * chunk)
                self.own[core, k, place, :] = part
                self.mine[core, k, place, :] = part.astype(BF)

    def pair_copy(self):
        return self.copy(self.mine.at[1 - self.plan.core], self.got_pair, 0, 0, (self.plan.mate, self.plan.c))

    def start_pair(self):
        if self.plan.pair == 2:
            self.pair_copy().start()

    def spread_copy(self, d):
        index, device = self.plan.peer(self.plan.ways[d])
        return self.copy(self.acc.at[index], self.got.at[d], 1, d, device)

    def start_spread(self):
        if self.plan.pair == 2:
            self.pair_copy().wait()
            self.acc[...] = (self.own[self.plan.core] + self.got_pair[...].astype(F32)).astype(BF)
        else:
            self.acc[...] = self.mine[0]
        for d in range(len(self.plan.ways)):
            self.spread_copy(d).start()

    def gather_copy(self, d):
        part = self.whole.at[self.plan.core, self.plan.chip]
        return self.copy(part, part, 2, d, self.plan.peer(self.plan.ways[d])[1])

    def back_copy(self, d, core):
        index = self.plan.chip if d == len(self.plan.ways) else self.plan.peer(self.plan.ways[d], -1)[0]
        part = self.whole.at[core, index]
        return self.copy(part, part, 3, d, (self.plan.mate, self.plan.c))

    def start_gather(self):
        plan = self.plan
        total = self.own[plan.core, plan.chip]
        if plan.pair == 2:
            total = total + self.got_pair[plan.chip].astype(F32)
        for d in range(len(plan.ways)):
            self.spread_copy(d).wait()
        for d in range(len(plan.ways)):
            total = total + self.got[d].astype(F32)
        self.whole[plan.core, plan.chip] = total.astype(BF)
        for d in range(len(plan.ways)):
            self.gather_copy(d).start()
        if plan.pair == 2:
            self.back_copy(len(plan.ways), plan.core).start()

    def start_back(self):
        plan = self.plan
        for d in reversed(range(len(plan.ways))):
            index = plan.peer(plan.ways[d], -1)[0]
            part = self.whole.at[plan.core, index]
            self.copy(part, part, 2, d, plan.peer(plan.ways[d], -1)[1]).wait_recv()
            if plan.pair == 2:
                self.back_copy(d, plan.core).start()

    def finish(self):
        plan = self.plan
        for d in range(len(plan.ways)):
            self.gather_copy(d).wait_send()
        if plan.pair == 2:
            for d in range(len(plan.ways) + 1):
                self.back_copy(d, plan.core).wait_send()
                self.back_copy(d, 1 - plan.core).wait_recv()


def slabs(sizes, chips):
    out, at = [], 0
    for size in sizes:
        chunk = up_to(-(-size // chips), 8)
        out.append((at, chunk))
        at += chunk
    return out


def slab_rows(sizes, chips):
    return sum(chunk for _, chunk in slabs(sizes, chips))


def summer_scratch(plan, sizes):
    rows, dma, n = slab_rows(sizes, plan.chips), pltpu.SemaphoreType.DMA, max(len(plan.ways), 1)
    full = (plan.chips, rows, plan.lanes)
    return [pltpu.VMEM((plan.pair,) + full, F32), pltpu.VMEM((plan.pair,) + full, BF), pltpu.VMEM(full, BF),
            pltpu.VMEM(full, BF), pltpu.VMEM((n, rows, plan.lanes), BF),
            dma((1,)), dma((1,)), dma((n,)), dma((n,)), dma((n,)), dma((n,)), dma((n + 1,)), dma((n + 1,))]


SUMMER_REFS = 13
UNITS, SIDE = 2, 256


NAMES = ("local", "halo", "features", "halo_first", "halo_second", "halo_third", "return_second", "return_third",
         "weight_first", "weight_second", "weight_third", "index_row", "labels")


def product(accs, lhs, rhs, depth, transpose=False):
    for k in depth:
        for q in range(UNITS):
            pltpu.matmul_push_rhs(rhs(k), staging_register=0, mxu_index=q, transpose=transpose)
            for i, acc in enumerate(accs[q]):
                pltpu.matmul_acc_lhs(acc, lhs(q, i, k), load_staged_rhs=0 if i == 0 else None)


def padded(value, rows, lanes=None):
    if value.shape[0] < rows:
        value = jnp.concatenate([value, jnp.zeros((rows - value.shape[0], value.shape[1]), value.dtype)], axis=0)
    if lanes is not None and value.shape[1] < lanes:
        value = jnp.concatenate([value, jnp.zeros((value.shape[0], lanes - value.shape[1]), value.dtype)], axis=1)
    return value


def span(k):
    return slice(k * SIDE, (k + 1) * SIDE)


def step_kernel(plan, tiles, early_sizes, late_sizes, *refs):
    count = len(NAMES)
    hbm = dict(zip(NAMES, refs[:count]))
    whole_early, whole_late, n2, n3, b2, b3 = refs[count:count + 6]
    (in_sem, local_i, halo_i, x_t, values_two, values_three, scaled_three, scaled_two, w1, w2, w3, index_row, labels,
     near_far, back, halo_t, hits_t, inverse, mixed_t, mixed_two, mixed_two_t, mixed_three, slope_one, slope_two, upstream,
     upstream_three_t, target_held, w3_wide, s2, s3, o2, o3, hsend, hrecv) = refs[count + 6:count + 40]
    rest = refs[count + 40:]
    early, late = (Summer(plan, sizes, *part[:5], whole, part[5:]) for sizes, part, whole in (
        (early_sizes, rest[:SUMMER_REFS], whole_early), (late_sizes, rest[SUMMER_REFS:], whole_late)))
    nodes, slots = local_i.shape[0], halo_i.shape[1]
    every, width, classes = nodes + slots, x_t.shape[0], w3.shape[0]
    plan.place()

    own, other = pl.ds(0, nodes), pl.ds(nodes, slots)
    tall = nodes // tiles
    tile = [slice(t * tall, (t + 1) * tall) for t in range(tiles)]
    targets = {"features": x_t.at[:, own], "halo_first": x_t.at[:, other], "halo_second": values_two.at[other],
               "halo_third": values_three.at[other], "return_second": scaled_two.at[other],
               "return_third": scaled_three.at[other], "weight_first": w1, "weight_second": w2, "weight_third": w3,
               "index_row": index_row, "labels": labels}
    loads = {}

    def load(key, src, dst):
        loads[key] = pltpu.make_async_copy(src, dst, in_sem.at[len(loads)])
        loads[key].start()

    for name in ("index_row", "labels", "features", "halo_first"):
        load(name, hbm[name], targets[name])
    for t in range(tiles):
        rows = pl.ds(t * tall, tall)
        load(("local", t), hbm["local"].at[rows], local_i.at[rows])
        load(("halo", t), hbm["halo"].at[rows], halo_i.at[rows])
        if t == 0:
            load("weight_first", hbm["weight_first"], w1)
    late_names = NAMES[4:8] + NAMES[9:11]
    for name in late_names:
        load(name, hbm[name], targets[name])

    halo_clear(plan, (n2, n3, b2, b3))
    plan.greet()
    early.clear()
    late.clear()
    loads["index_row"].wait()
    back[:, other] = jnp.where(lax.broadcasted_iota(jnp.int32, (nodes, slots), 0) == index_row[...], 1.0, 0.0).astype(BF)
    hits_t[...] = back[:, other].T
    loads["labels"].wait()
    wide = target_held.shape[1]
    target_held[...] = jnp.where(lax.broadcasted_iota(jnp.int32, (wide, nodes), 0) == labels[...], 1.0, 0.0).T
    w3_wide[...] = jnp.zeros_like(w3_wide)

    tail = up_to(width, 16 * UNITS) - UNITS * SIDE * (width // (UNITS * SIDE))
    body = width // (UNITS * SIDE)
    strip = tail // UNITS

    def first_rows(q, i):
        return ((q + UNITS * i) * SIDE, SIDE) if i < body else (UNITS * SIDE * body + q * strip, strip)

    def first_layer(*accs):
        mix = [[accs[q + UNITS * (i + (body + 1) * b)] for q in range(UNITS) for i in range(body + 1)] for b in range(2)]
        mix = [[m[q * (body + 1):(q + 1) * (body + 1)] for q in range(UNITS)] for m in mix]
        pres = accs[2 * UNITS * (body + 1):]
        for acc in accs:
            pltpu.matmul_pop(acc)

        def gather(t):
            loads[("local", t)].wait()
            loads[("halo", t)].wait()
            near, far = local_i[tile[t], :].astype(F32), halo_i[tile[t], :].astype(F32)
            total = 1.0 + jnp.sum(near, axis=1, keepdims=True) + jnp.sum(far, axis=1, keepdims=True)
            near_far[tile[t], own] = near.astype(BF)
            near_far[tile[t], other] = far.astype(BF)
            square = near[:, tile[t]]
            here = lax.broadcasted_iota(jnp.int32, square.shape, 0) == lax.broadcasted_iota(jnp.int32, square.shape, 1)
            near_far[tile[t], tile[t]] = jnp.where(here, square + 1.0, square).astype(BF)
            inverse[tile[t], :] = jnp.broadcast_to(1.0 / total, (tall, inverse.shape[1]))
            if t == 0:
                loads["features"].wait()
                loads["halo_first"].wait()
            product(mix[t % 2], lambda q, i, k: padded(x_t[slice(first_rows(q, i)[0], min(sum(first_rows(q, i)), width)), span(k)], first_rows(q, i)[1]),
                    lambda k: near_far[tile[t], span(k)], range(every // SIDE), True)

        def settle(t):
            across = inverse[tile[t], :128].T[0:1]
            for i in range(body + 1):
                for q in range(UNITS):
                    start, size = first_rows(q, i)
                    mixed_t[start:start + size, tile[t]] = (pltpu.matmul_pop(mix[t % 2][q][i]) * across).astype(BF)
            back[own, tile[t]] = near_far[tile[t], own].T
            halo_t[:, tile[t]] = near_far[tile[t], other].T
            if t == 0:
                loads["weight_first"].wait()
            pre_acc = [pres[UNITS * (t % 2) + q] for q in range(UNITS)]
            half = tall // UNITS
            depth = -(-width // SIDE)
            turned = [mixed_t[k * SIDE:min((k + 1) * SIDE, mixed_t.shape[0]), tile[t]].T for k in range(depth)]
            product([[acc] for acc in pre_acc], lambda q, i, k: padded(turned[k][q * half:(q + 1) * half], half, SIDE),
                    lambda k: padded(w1[k * SIDE:min((k + 1) * SIDE, width), :], SIDE), range(depth))
            for q in range(UNITS):
                rows = slice(t * tall + q * half, t * tall + (q + 1) * half)
                pre = pltpu.matmul_pop(pre_acc[q])
                sigma = jax.nn.sigmoid(pre)
                values_two[rows, :] = (pre * sigma).astype(BF)
                slope_one[rows, :] = slope(pre, sigma)

        for t in range(tiles):
            gather(t)
            if t > 0:
                settle(t - 1)
        settle(tiles - 1)

    def accs_of(sizes):
        return [pltpu.ACC(q)((size, SIDE), F32) for size in sizes for q in range(UNITS)]

    sizes = ([SIDE] * body + [strip]) * 2 + [tall // UNITS] * 2
    pl.run_scoped(first_layer, *accs_of(sizes))

    for name in late_names:
        loads[name].wait()
    w3_wide[0:classes, :] = w3[...]
    order = list(range(nodes // SIDE, every // SIDE)) + list(range(nodes // SIDE))

    def rest_of_step(*accs):
        held = [[accs[q + UNITS * i] for i in range(6)] for q in range(UNITS)]
        first, second = [p[0:2] for p in held], [p[2:3] for p in held]
        middle, small, small_late = ([p[i] for p in held] for i in (3, 4, 5))

        def at(q, i):
            return slice((q + UNITS * i) * SIDE, (q + UNITS * i + 1) * SIDE)

        def tall_product(sets, left, right, depth, transpose=False, pieces=2):
            for i in range(pieces):
                product([[sets[q][i]] for q in range(UNITS)], lambda q, _, k: left[at(q, i), span(k)],
                        lambda k: right(k), depth, transpose)

        def pops(sets, use, pieces=2):
            for i in range(pieces):
                for q in range(UNITS):
                    use(at(q, i), pltpu.matmul_pop(sets[q][i]))

        def keep_mixed(mixed, mixed_turned):
            def use(rows, value):
                out = (value * inverse[rows, :]).astype(BF)
                mixed[rows, :] = out
                if mixed_turned is not None:
                    mixed_turned[:, rows] = out.T
            return use

        def keep(out):
            def use(rows, value):
                out[rows, :] = value.astype(BF)
            return use

        def keep_scaled(out):
            def use(rows, value):
                out[rows, :] = (value * inverse[rows, :]).astype(BF)
            return use

        tall_product(first, near_far, lambda k: values_two[span(k), :], order)
        tall_product(second, hits_t, lambda k: values_two[span(k), :], range(nodes // SIDE), pieces=1)
        pops(first, keep_mixed(mixed_two, mixed_two_t))
        tall_product(first, mixed_two, lambda k: w2[...], range(1))
        pops(second, keep(s2), pieces=1)

        def activate(rows, pre):
            sigma = jax.nn.sigmoid(pre)
            values_three[rows, :] = (pre * sigma).astype(BF)
            slope_two[rows, :] = slope(pre, sigma)

        pops(first, activate)
        halo_start(plan, s2, n2, hsend, hrecv, 0)
        tall_product(first, near_far, lambda k: values_three[span(k), :], order)
        tall_product(second, hits_t, lambda k: values_three[span(k), :], range(nodes // SIDE), pieces=1)
        pops(first, keep_mixed(mixed_three, None))
        tall_product(first, mixed_three, lambda k: w3_wide[...], range(1), True)
        pops(second, keep(s3), pieces=1)
        ups = {}

        def soften(rows, logits):
            logits = logits[:, :wide]
            inside = lax.broadcasted_iota(jnp.int32, logits.shape, 1) < classes
            expo = jnp.where(inside, jnp.exp(logits), 0.0)
            probs = expo / jnp.sum(expo, axis=1, keepdims=True)
            up = ((probs - target_held[rows, :]) / nodes).astype(BF)
            upstream_three_t[:, rows] = up.T
            ups[rows.start] = padded(up, up.shape[0], SIDE)

        pops(first, soften)
        for i in range(2):
            product([[first[q][i]] for q in range(UNITS)], lambda q, _, k: ups[at(q, i).start], lambda k: w3_wide[...], range(1))
        pops(first, keep_scaled(scaled_three))
        halo_start(plan, s3, n3, hsend, hrecv, 1)
        tall_product(first, back, lambda k: scaled_three[span(k), :], order)
        stripes = nodes // SIDE // UNITS
        for k in range(stripes):
            for q in range(UNITS):
                pltpu.matmul_push_rhs(mixed_three[span(q * stripes + k), :], staging_register=0, mxu_index=q)
                pltpu.matmul_acc_lhs(small[q], upstream_three_t[0:small_rows, span(q * stripes + k)], load_staged_rhs=0)
        tall_product(second, halo_t, lambda k: scaled_three[span(k), :], range(nodes // SIDE), pieces=1)

        def climb(slopes):
            def use(rows, value):
                upstream[rows, :] = (value * slopes[rows, :]).astype(BF)
            return use

        pops(first, climb(slope_two))
        tall_product(first, upstream, lambda k: w2[...], range(1), True)
        early.put(1, pltpu.matmul_pop(small[0]) + pltpu.matmul_pop(small[1]))
        pops(second, keep(o3), pieces=1)
        half = mixed_two_t.shape[0] // UNITS
        for k in range(nodes // SIDE):
            for q in range(UNITS):
                pltpu.matmul_push_rhs(upstream[span(k), :], staging_register=0, mxu_index=q)
                pltpu.matmul_acc_lhs(middle[q], mixed_two_t[q * half:(q + 1) * half, span(k)], load_staged_rhs=0)
        pops(first, keep_scaled(scaled_two))
        for q in range(UNITS):
            early.put(0, pltpu.matmul_pop(middle[q]), q * half)
        early.start_pair()
        halo_start(plan, o3, b3, hsend, hrecv, 2)
        tall_product(first, back, lambda k: scaled_two[span(k), :], order)
        tall_product(second, halo_t, lambda k: scaled_two[span(k), :], range(nodes // SIDE), pieces=1)
        early.start_spread()
        pops(first, climb(slope_one))
        product([first[q][:body] + [small_late[q]] for q in range(UNITS)],
                lambda q, i, k: mixed_t[slice(first_rows(q, i)[0], sum(first_rows(q, i))), span(k)],
                lambda k: upstream[span(k), :], range(nodes // SIDE))
        pops(second, keep(o2), pieces=1)
        for i in range(body + 1):
            for q in range(UNITS):
                late.put(0, pltpu.matmul_pop((first[q][:body] + [small_late[q]])[i]), first_rows(q, i)[0])
        late.start_pair()

    small_rows = up_to(classes, 16)
    pl.run_scoped(rest_of_step, *accs_of([SIDE] * 3 + [mixed_two_t.shape[0] // UNITS, small_rows, strip]))
    late.start_spread()
    early.start_gather()
    halo_start(plan, o2, b2, hsend, hrecv, 3)
    late.start_gather()
    early.start_back()
    late.start_back()
    early.finish()
    late.finish()
    for way, (src, dst) in enumerate(((s2, n2), (s3, n3), (o3, b3), (o2, b2))):
        halo_finish(plan, src, dst, hsend, hrecv, way)


def finish_kernel(plan, early_sizes, late_sizes, whole_early, whole_late, n2, n3, b2, b3, g1, g2, g3, m2, m3, a2, a3, h1, h2, h3, sem):
    copies = [pltpu.make_async_copy(src, dst, sem.at[i]) for i, (src, dst) in enumerate(((n2, m2), (n3, m3), (b2, a2), (b3, a3)))]
    for copy in copies:
        copy.start()
    for i, (ref, out, whole, sizes, part) in enumerate((
            (h1, g1, whole_late, late_sizes, 0), (h2, g2, whole_early, early_sizes, 0), (h3, g3, whole_early, early_sizes, 1))):
        at, chunk = slabs(sizes, plan.chips)[part]
        for core in range(plan.pair):
            for k in range(-(-ref.shape[0] // chunk)):
                rows = min(chunk, ref.shape[0] - k * chunk)
                ref[k * chunk:k * chunk + rows, core * plan.lanes:(core + 1) * plan.lanes] = whole[core, k, at:at + rows, :].astype(F32)
        copies.append(pltpu.make_async_copy(ref, out, sem.at[4 + i]))
        copies[-1].start()
    for copy in copies:
        copy.wait()


def per_device(mesh, features, local_mask, halo_mask, boundary_index, labels, halo_first, halo_second, halo_third,
               return_second, return_third, weight_first, weight_second, weight_third):
    features, local_mask, halo_mask = features[0, 0], local_mask[0, 0], halo_mask[0, 0]
    index, labels = boundary_index[0, 0], labels[0, 0]
    halo_first, halo_second, halo_third = halo_first[0, 0], halo_second[0, 0], halo_third[0, 0]
    return_second, return_third = return_second[0, 0], return_third[0, 0]
    nodes, width = features.shape
    slots, hidden, classes = index.shape[0], weight_first.shape[1], weight_third.shape[1]
    plan = Plan(mesh, hidden)
    early_sizes, late_sizes = (weight_second.shape[0], classes), (width,)
    tiles = 4 if nodes % 512 == 0 else 1
    values = (local_mask, halo_mask, features.T, halo_first.T, halo_second, halo_third, return_second, return_third,
              weight_first, weight_second, weight_third.T, index[None, :], labels[None, :])
    values = tuple(pltpu.with_memory_space_constraint(v, pltpu.HBM) for v in values)
    vmem, anywhere = pl.BlockSpec(memory_space=pltpu.VMEM), pl.BlockSpec(memory_space=pl.ANY)
    dma = pltpu.SemaphoreType.DMA
    block = jax.ShapeDtypeStruct((slots, hidden), BF)
    every = nodes + slots

    def held(value):
        return pltpu.VMEM(value.shape, value.dtype)

    done = pl.pallas_call(
        functools.partial(step_kernel, plan, tiles, early_sizes, late_sizes),
        out_shape=tuple(jax.ShapeDtypeStruct((plan.pair, plan.chips, slab_rows(sizes, plan.chips), plan.lanes), BF)
                        for sizes in (early_sizes, late_sizes)) + (block,) * 4,
        in_specs=[anywhere] * len(values), out_specs=(vmem,) * 6,
        scratch_shapes=[
            dma((len(values) + 2 * tiles,)), held(local_mask), held(halo_mask), pltpu.VMEM((width, every), BF),
            pltpu.VMEM((every, hidden), BF), pltpu.VMEM((every, hidden), BF), pltpu.VMEM((every, hidden), BF),
            pltpu.VMEM((every, hidden), BF), held(values[8]), held(values[9]), held(values[10]), held(values[11]), held(values[12]),
            pltpu.VMEM((nodes, every), BF), pltpu.VMEM((nodes, every), BF), pltpu.VMEM((slots, nodes), BF),
            pltpu.VMEM((slots, nodes), BF), pltpu.VMEM((nodes, hidden), F32), pltpu.VMEM((up_to(width, 16 * UNITS), nodes), BF),
            pltpu.VMEM((nodes, hidden), BF), pltpu.VMEM((hidden, nodes), BF), pltpu.VMEM((nodes, hidden), BF), pltpu.VMEM((nodes, hidden), F32),
            pltpu.VMEM((nodes, hidden), F32), pltpu.VMEM((nodes, hidden), BF), pltpu.VMEM((up_to(classes, 128), nodes), BF),
            pltpu.VMEM((nodes, up_to(classes, 128)), F32), pltpu.VMEM((SIDE, hidden), BF)]
        + [pltpu.VMEM((slots, hidden), BF)] * 4 + [dma((4, 4)), dma((4, 4))]
        + summer_scratch(plan, early_sizes) + summer_scratch(plan, late_sizes),
        compiler_params=pltpu.CompilerParams(collective_id=0, has_side_effects=True, vmem_limit_bytes=40 * 2**20),
        name="step",
    )(*values)
    grads = ((weight_first.shape, F32), (weight_second.shape, F32), (weight_third.shape[::-1], F32))
    out = pl.pallas_call(
        functools.partial(finish_kernel, plan, early_sizes, late_sizes),
        out_shape=tuple(jax.ShapeDtypeStruct(*g) for g in grads) + (block,) * 4,
        in_specs=[vmem] * 6, out_specs=(anywhere,) * 7,
        scratch_shapes=[pltpu.VMEM(*g) for g in grads] + [dma((7,))],
        compiler_params=pltpu.CompilerParams(vmem_limit_bytes=16 * 2**20), name="finish",
    )(*done)
    return (out[0], out[1], out[2].T) + tuple(v[None, None] for v in out[3:])


def solution(mesh):
    wide, flat, copied = P("row", "col", None, None), P("row", "col", None), P()
    return jax.shard_map(
        functools.partial(per_device, mesh), mesh=mesh,
        in_specs=(wide, wide, wide, flat, flat, wide, wide, wide, wide, wide, copied, copied, copied),
        out_specs=(copied, copied, copied, wide, wide, wide, wide),
        check_vma=False,
    )
```

```python
import functools

import jax
import jax.numpy as jnp
from jax import lax
from jax.experimental import pallas as pl
from jax.experimental.pallas import tpu as pltpu
from jax.sharding import PartitionSpec as P

MESH = pl.DeviceIdType.MESH
BF = jnp.bfloat16
F32 = jnp.float32


def up_to(value, step):
    return -(-value // step) * step


def dot(a, b, dims=((1,), (0,))):
    return lax.dot_general(a, b, (dims, ((), ())), preferred_element_type=F32)


def slope(pre, sigma):
    return sigma * (1.0 + pre * (1.0 - sigma))


class Plan:
    def __init__(self, mesh, hidden):
        self.n_row, self.n_col = mesh.shape["row"], mesh.shape["col"]
        self.pair = 2 if self.n_row % 2 == 0 else 1
        self.deep = self.n_row // self.pair
        self.chips = self.deep * self.n_col
        self.lanes = hidden // self.pair
        deep = sorted(range(self.deep), key=lambda d: -min(d, self.deep - d))
        cols = sorted(range(self.n_col), key=lambda d: -min(d, self.n_col - d))
        self.ways = [(dz, dc) for dz in deep for dc in cols if dz or dc]

    def place(self):
        self.r, self.c = lax.axis_index("row"), lax.axis_index("col")
        self.core, self.z = self.r % self.pair, self.r // self.pair
        self.mate = self.r + 1 - 2 * self.core
        self.chip = self.z * self.n_col + self.c

    def peer(self, way, sign=1):
        z = (self.z + sign * way[0] + self.deep) % self.deep
        c = (self.c + sign * way[1] + self.n_col) % self.n_col
        return z * self.n_col + c, (z * self.pair + self.core, c)

    def greet(self):
        barrier = pltpu.get_barrier_semaphore()

        def hello(device):
            pl.semaphore_signal(barrier, inc=1, device_id=device, device_id_type=MESH)

        count = 0
        if self.pair == 2:
            hello((self.mate, self.c))
            count += 1
        for way in self.ways:
            hello(self.peer(way)[1])
            count += 1
        for step, there in self.far_rows():
            @pl.when(there)
            def _():
                hello((self.r + step, self.c))
        for _, there in self.far_rows():
            count = count + jnp.where(there, 1, 0)
        return lambda: pl.semaphore_wait(barrier, count)

    def far_rows(self):
        if self.pair == 2:
            return ((-1, jnp.logical_and(self.core == 0, self.r > 0)),
                    (1, jnp.logical_and(self.core == 1, self.r < self.n_row - 1)))
        return ()

    def edges(self):
        r, c = self.r, self.c
        return (((r - 1, c), 1, r > 0), ((r + 1, c), 0, r < self.n_row - 1),
                ((r, c - 1), 3, c > 0), ((r, c + 1), 2, c < self.n_col - 1))


def halo_copy(plan, k, src, dst, send, recv, way):
    bound = src.shape[0] // 4
    device, slot, there = plan.edges()[k]
    copy = pltpu.make_async_remote_copy(
        src_ref=src.at[pl.ds(k * bound, bound)], dst_ref=dst.at[pl.ds(slot * bound, bound)],
        send_sem=send.at[way, k], recv_sem=recv.at[way, slot], device_id=device, device_id_type=MESH)
    return copy, slot, there


def halo_start(plan, src, dst, send, recv, way):
    bound = src.shape[0] // 4
    for k in range(4):
        copy, _, there = halo_copy(plan, k, src, dst, send, recv, way)

        @pl.when(there)
        def _():
            copy.start()


def halo_clear(plan, dsts):
    bound = dsts[0].shape[0] // 4
    for k in range(4):
        @pl.when(jnp.logical_not(plan.edges()[k][2]))
        def _():
            for dst in dsts:
                dst[pl.ds(k * bound, bound), :] = jnp.zeros((bound, dst.shape[1]), dst.dtype)


def halo_finish(plan, src, dst, send, recv, way):
    bound = src.shape[0] // 4
    for k in range(4):
        copy, _, there = halo_copy(plan, k, src, dst, send, recv, way)
        arrival = pltpu.make_async_remote_copy(
            src_ref=src.at[pl.ds(k * bound, bound)], dst_ref=dst.at[pl.ds(k * bound, bound)],
            send_sem=send.at[way, k], recv_sem=recv.at[way, k], device_id=plan.edges()[k][0], device_id_type=MESH)

        @pl.when(there)
        def _():
            copy.wait_send()
            arrival.wait_recv()


class Summer:
    def __init__(self, plan, sizes, own, mine, got_pair, acc, got, whole, sems):
        self.plan, self.sizes, self.own, self.mine, self.got_pair = plan, sizes, own, mine, got_pair
        self.acc, self.got, self.whole, self.sems = acc, got, whole, sems

    def copy(self, src, dst, kind, d, device):
        return pltpu.make_async_remote_copy(
            src_ref=src, dst_ref=dst, send_sem=self.sems[2 * kind].at[d], recv_sem=self.sems[2 * kind + 1].at[d],
            device_id=device, device_id_type=MESH)

    def clear(self):
        self.own[...] = jnp.zeros_like(self.own)
        self.mine[...] = jnp.zeros_like(self.mine)

    def put(self, i, value, row=0):
        at, chunk = slabs(self.sizes, self.plan.chips)[i]
        end = min(row + value.shape[0], self.sizes[i])
        for k in range(row // chunk, -(-end // chunk)):
            low, high = max(row, k * chunk), min(end, (k + 1) * chunk)
            for core in range(self.plan.pair):
                part = value[low - row:high - row, core * self.plan.lanes:(core + 1) * self.plan.lanes]
                place = slice(at + low - k * chunk, at + high - k * chunk)
                self.own[core, k, place, :] = part
                self.mine[core, k, place, :] = part.astype(BF)

    def pair_copy(self):
        return self.copy(self.mine.at[1 - self.plan.core], self.got_pair, 0, 0, (self.plan.mate, self.plan.c))

    def start_pair(self):
        if self.plan.pair == 2:
            self.pair_copy().start()

    def spread_copy(self, d):
        index, device = self.plan.peer(self.plan.ways[d])
        return self.copy(self.acc.at[index], self.got.at[d], 1, d, device)

    def start_spread(self):
        if self.plan.pair == 2:
            self.pair_copy().wait()
            self.acc[...] = (self.own[self.plan.core] + self.got_pair[...].astype(F32)).astype(BF)
        else:
            self.acc[...] = self.mine[0]
        for d in range(len(self.plan.ways)):
            self.spread_copy(d).start()

    def gather_copy(self, d):
        part = self.whole.at[self.plan.core, self.plan.chip]
        return self.copy(part, part, 2, d, self.plan.peer(self.plan.ways[d])[1])

    def back_copy(self, d, core):
        index = self.plan.chip if d == len(self.plan.ways) else self.plan.peer(self.plan.ways[d], -1)[0]
        part = self.whole.at[core, index]
        return self.copy(part, part, 3, d, (self.plan.mate, self.plan.c))

    def start_gather(self):
        plan = self.plan
        total = self.own[plan.core, plan.chip]
        if plan.pair == 2:
            total = total + self.got_pair[plan.chip].astype(F32)
        for d in range(len(plan.ways)):
            self.spread_copy(d).wait()
        for d in range(len(plan.ways)):
            total = total + self.got[d].astype(F32)
        self.whole[plan.core, plan.chip] = total.astype(BF)
        for d in range(len(plan.ways)):
            self.gather_copy(d).start()
        if plan.pair == 2:
            self.back_copy(len(plan.ways), plan.core).start()

    def start_back(self):
        plan = self.plan
        for d in reversed(range(len(plan.ways))):
            index = plan.peer(plan.ways[d], -1)[0]
            part = self.whole.at[plan.core, index]
            self.copy(part, part, 2, d, plan.peer(plan.ways[d], -1)[1]).wait_recv()
            if plan.pair == 2:
                self.back_copy(d, plan.core).start()

    def finish(self):
        plan = self.plan
        for d in range(len(plan.ways)):
            self.gather_copy(d).wait_send()
        if plan.pair == 2:
            for d in range(len(plan.ways) + 1):
                self.back_copy(d, plan.core).wait_send()
                self.back_copy(d, 1 - plan.core).wait_recv()


def slabs(sizes, chips):
    out, at = [], 0
    for size in sizes:
        chunk = up_to(-(-size // chips), 8)
        out.append((at, chunk))
        at += chunk
    return out


def slab_rows(sizes, chips):
    return sum(chunk for _, chunk in slabs(sizes, chips))


def summer_scratch(plan, sizes):
    rows, dma, n = slab_rows(sizes, plan.chips), pltpu.SemaphoreType.DMA, max(len(plan.ways), 1)
    full = (plan.chips, rows, plan.lanes)
    return [pltpu.VMEM((plan.pair,) + full, F32), pltpu.VMEM((plan.pair,) + full, BF), pltpu.VMEM(full, BF),
            pltpu.VMEM(full, BF), pltpu.VMEM((n, rows, plan.lanes), BF),
            dma((1,)), dma((1,)), dma((n,)), dma((n,)), dma((n,)), dma((n,)), dma((n + 1,)), dma((n + 1,))]


SUMMER_REFS = 13
LATE_AT = 1
UNITS, SIDE = 2, 256


NAMES = ("local", "halo", "features", "halo_first", "halo_second", "halo_third", "return_second", "return_third",
         "weight_first", "weight_second", "weight_third", "index_row", "labels")


def product(accs, lhs, rhs, depth, transpose=False):
    for k in depth:
        for q in range(UNITS):
            pltpu.matmul_push_rhs(rhs(k), staging_register=0, mxu_index=q, transpose=transpose)
            for i, acc in enumerate(accs[q]):
                pltpu.matmul_acc_lhs(acc, lhs(q, i, k), load_staged_rhs=0 if i == 0 else None)


def padded(value, rows, lanes=None):
    if value.shape[0] < rows:
        value = jnp.concatenate([value, jnp.zeros((rows - value.shape[0], value.shape[1]), value.dtype)], axis=0)
    if lanes is not None and value.shape[1] < lanes:
        value = jnp.concatenate([value, jnp.zeros((value.shape[0], lanes - value.shape[1]), value.dtype)], axis=1)
    return value


def span(k):
    return slice(k * SIDE, (k + 1) * SIDE)


def step_kernel(plan, tiles, early_sizes, late_sizes, *refs):
    count = len(NAMES)
    hbm = dict(zip(NAMES, refs[:count]))
    whole_early, whole_late, n2, n3, b2, b3 = refs[count:count + 6]
    (in_sem, local_i, halo_i, x_t, values_two, values_three, scaled_three, scaled_two, w1, w2, w3, index_row, labels,
     near_far, back, halo_t, hits_t, inverse, mixed_t, mixed_two, mixed_two_t, mixed_three, slope_one, slope_two, upstream,
     upstream_three_t, target_held, w3_wide, s2, s3, o2, o3, hsend, hrecv) = refs[count + 6:count + 40]
    rest = refs[count + 40:]
    early, late = (Summer(plan, sizes, *part[:5], whole, part[5:]) for sizes, part, whole in (
        (early_sizes, rest[:SUMMER_REFS], whole_early), (late_sizes, rest[SUMMER_REFS:], whole_late)))
    nodes, slots = local_i.shape[0], halo_i.shape[1]
    every, width, classes = nodes + slots, x_t.shape[0], w3.shape[0]
    plan.place()

    own, other = pl.ds(0, nodes), pl.ds(nodes, slots)
    tall = nodes // tiles
    tile = [slice(t * tall, (t + 1) * tall) for t in range(tiles)]
    targets = {"features": (x_t, 1, 0), "halo_first": (x_t, 1, nodes), "halo_second": (values_two, 0, nodes),
               "halo_third": (values_three, 0, nodes), "return_second": (scaled_two, 0, nodes),
               "return_third": (scaled_three, 0, nodes), "weight_first": (w1, 0, 0), "weight_second": (w2, 0, 0),
               "weight_third": (w3, 0, 0), "index_row": (index_row, 0, 0), "labels": (labels, 0, 0)}
    slot = {}

    class Load:
        def __init__(self, key):
            self.key = key

        def copy(self):
            index = slot.setdefault(self.key, len(slot))
            if isinstance(self.key, tuple):
                name, t = self.key
                rows = pl.ds(t * tall, tall)
                return pltpu.make_async_copy(hbm[name].at[rows], {"local": local_i, "halo": halo_i}[name].at[rows], in_sem.at[index])
            ref, axis, start = targets[self.key]
            part = pl.ds(start, hbm[self.key].shape[axis])
            return pltpu.make_async_copy(hbm[self.key], ref.at[:, part] if axis else ref.at[part], in_sem.at[index])

        def start(self):
            self.copy().start()

        def wait(self):
            self.copy().wait()

    loads = {}

    def load(key):
        loads[key] = Load(key)
        loads[key].start()

    late_names = ("halo_second", "halo_third", "return_third", "return_second", "weight_third")

    def load_tile(t):
        load(("local", t))
        load(("halo", t))

    def load_named(names):
        for name in names:
            load(name)

    load_tile(0)
    first_names = ("features", "halo_first", "weight_first", "index_row", "labels", "weight_second")
    load_named(first_names)
    for t in range(1, tiles):
        load_tile(t)

    halo_clear(plan, (n2, n3, b2, b3))
    met = plan.greet()
    early.clear()
    late.clear()
    wide = target_held.shape[1]

    def mark():
        back[:, other] = jnp.where(lax.broadcasted_iota(jnp.int32, (nodes, slots), 0) == index_row[...], 1.0, 0.0).astype(BF)
        hits_t[...] = back[:, other].T
        target_held[...] = jnp.where(lax.broadcasted_iota(jnp.int32, (wide, nodes), 0) == labels[...], 1.0, 0.0).T
        w3_wide[...] = jnp.zeros_like(w3_wide)

    tail = up_to(width, 16 * UNITS) - UNITS * SIDE * (width // (UNITS * SIDE))
    body = width // (UNITS * SIDE)
    strip = tail // UNITS

    def first_rows(q, i):
        return ((q + UNITS * i) * SIDE, SIDE) if i < body else (UNITS * SIDE * body + q * strip, strip)

    def first_layer(*accs):
        mix = [[accs[q + UNITS * (i + (body + 1) * b)] for q in range(UNITS) for i in range(body + 1)] for b in range(2)]
        mix = [[m[q * (body + 1):(q + 1) * (body + 1)] for q in range(UNITS)] for m in mix]
        pres = accs[2 * UNITS * (body + 1):]
        for acc in accs:
            pltpu.matmul_pop(acc)

        def gather(t):
            loads[("local", t)].wait()
            loads[("halo", t)].wait()
            if t == LATE_AT:
                load_named(late_names)
            if t == tiles - 1:
                loads[late_names[0]].wait()
            near, far = local_i[tile[t], :].astype(F32), halo_i[tile[t], :].astype(F32)
            total = 1.0 + jnp.sum(near, axis=1, keepdims=True) + jnp.sum(far, axis=1, keepdims=True)
            near_far[tile[t], own] = near.astype(BF)
            near_far[tile[t], other] = far.astype(BF)
            square = near[:, tile[t]]
            here = lax.broadcasted_iota(jnp.int32, square.shape, 0) == lax.broadcasted_iota(jnp.int32, square.shape, 1)
            near_far[tile[t], tile[t]] = jnp.where(here, square + 1.0, square).astype(BF)
            inverse[tile[t], :] = jnp.broadcast_to(1.0 / total, (tall, inverse.shape[1]))

        def mix_tile(t):
            product(mix[t % 2], lambda q, i, k: padded(x_t[slice(first_rows(q, i)[0], min(sum(first_rows(q, i)), width)), span(k)], first_rows(q, i)[1]),
                    lambda k: near_far[tile[t], span(k)], range(every // SIDE), True)

        def settle(t):
            pre_acc = [pres[UNITS * (t % 2) + q] for q in range(UNITS)]
            half = tall // UNITS
            across = inverse[tile[t], :128].T[0:1]
            for i in range(body + 1):
                for q in range(UNITS):
                    start, size = first_rows(q, i)
                    mixed_t[start:start + size, tile[t]] = (pltpu.matmul_pop(mix[t % 2][q][i]) * across).astype(BF)
            back[own, tile[t]] = near_far[tile[t], own].T
            halo_t[:, tile[t]] = near_far[tile[t], other].T
            depth = -(-width // SIDE)
            turned = [mixed_t[k * SIDE:min((k + 1) * SIDE, mixed_t.shape[0]), tile[t]].T for k in range(depth)]
            product([[acc] for acc in pre_acc], lambda q, i, k: padded(turned[k][q * half:(q + 1) * half], half, SIDE),
                    lambda k: padded(w1[k * SIDE:min((k + 1) * SIDE, width), :], SIDE), range(depth))

        def close(t):
            half = tall // UNITS
            for q in range(UNITS):
                rows = slice(t * tall + q * half, t * tall + (q + 1) * half)
                pre = pltpu.matmul_pop(pres[UNITS * (t % 2) + q])
                sigma = jax.nn.sigmoid(pre)
                values_two[rows, :] = (pre * sigma).astype(BF)
                slope_one[rows, :] = slope(pre, sigma)

        for t in range(tiles):
            gather(t)
            if t == 0:
                for name in first_names:
                    loads[name].wait()
            mix_tile(t)
            if t == 0:
                mark()
            if t > 1:
                close(t - 2)
            if t > 0:
                settle(t - 1)
        if tiles > 1:
            close(tiles - 2)
        settle(tiles - 1)
        close(tiles - 1)

    def accs_of(sizes):
        return [pltpu.ACC(q)((size, SIDE), F32) for size in sizes for q in range(UNITS)]

    sizes = ([SIDE] * body + [strip]) * 2 + [tall // UNITS] * 2
    pl.run_scoped(first_layer, *accs_of(sizes))

    order = list(range(nodes // SIDE, every // SIDE)) + list(range(nodes // SIDE))

    def rest_of_step(*accs):
        held = [[accs[q + UNITS * i] for i in range(6)] for q in range(UNITS)]
        first, second = [p[0:2] for p in held], [p[2:3] for p in held]
        middle, small, small_late = ([p[i] for p in held] for i in (3, 4, 5))

        def at(q, i):
            return slice((q + UNITS * i) * SIDE, (q + UNITS * i + 1) * SIDE)

        def tall_product(sets, left, right, depth, transpose=False, pieces=2):
            for i in range(pieces):
                product([[sets[q][i]] for q in range(UNITS)], lambda q, _, k: left[at(q, i), span(k)],
                        lambda k: right(k), depth, transpose)

        def pops(sets, use, pieces=2):
            for i in range(pieces):
                for q in range(UNITS):
                    use(at(q, i), pltpu.matmul_pop(sets[q][i]))

        def keep_mixed(mixed, mixed_turned):
            def use(rows, value):
                out = (value * inverse[rows, :]).astype(BF)
                mixed[rows, :] = out
                if mixed_turned is not None:
                    mixed_turned[:, rows] = out.T
            return use

        def keep(out):
            def use(rows, value):
                out[rows, :] = value.astype(BF)
            return use

        def keep_scaled(out):
            def use(rows, value):
                out[rows, :] = (value * inverse[rows, :]).astype(BF)
            return use

        tall_product(first, near_far, lambda k: values_two[span(k), :], order)
        tall_product(second, hits_t, lambda k: values_two[span(k), :], range(nodes // SIDE), pieces=1)
        pops(first, keep_mixed(mixed_two, mixed_two_t))
        tall_product(first, mixed_two, lambda k: w2[...], range(1))
        pops(second, keep(s2), pieces=1)

        def activate(rows, pre):
            sigma = jax.nn.sigmoid(pre)
            values_three[rows, :] = (pre * sigma).astype(BF)
            slope_two[rows, :] = slope(pre, sigma)

        pops(first, activate)
        for name in late_names[1:]:
            loads[name].wait()
        w3_wide[0:classes, :] = w3[...]
        met()
        halo_start(plan, s2, n2, hsend, hrecv, 0)
        tall_product(first, near_far, lambda k: values_three[span(k), :], order)
        tall_product(second, hits_t, lambda k: values_three[span(k), :], range(nodes // SIDE), pieces=1)
        pops(first, keep_mixed(mixed_three, None))
        tall_product(first, mixed_three, lambda k: w3_wide[...], range(1), True)
        pops(second, keep(s3), pieces=1)
        ups = {}

        def soften(rows, logits):
            logits = logits[:, :wide]
            inside = lax.broadcasted_iota(jnp.int32, logits.shape, 1) < classes
            expo = jnp.where(inside, jnp.exp(logits), 0.0)
            probs = expo / jnp.sum(expo, axis=1, keepdims=True)
            up = ((probs - target_held[rows, :]) / nodes).astype(BF)
            upstream_three_t[:, rows] = up.T
            ups[rows.start] = padded(up, up.shape[0], SIDE)

        pops(first, soften)
        for i in range(2):
            product([[first[q][i]] for q in range(UNITS)], lambda q, _, k: ups[at(q, i).start], lambda k: w3_wide[...], range(1))
        pops(first, keep_scaled(scaled_three))
        halo_start(plan, s3, n3, hsend, hrecv, 1)
        tall_product(first, back, lambda k: scaled_three[span(k), :], order)
        stripes = nodes // SIDE // UNITS
        for k in range(stripes):
            for q in range(UNITS):
                pltpu.matmul_push_rhs(mixed_three[span(q * stripes + k), :], staging_register=0, mxu_index=q)
                pltpu.matmul_acc_lhs(small[q], upstream_three_t[0:small_rows, span(q * stripes + k)], load_staged_rhs=0)
        tall_product(second, halo_t, lambda k: scaled_three[span(k), :], range(nodes // SIDE), pieces=1)

        def climb(slopes):
            def use(rows, value):
                upstream[rows, :] = (value * slopes[rows, :]).astype(BF)
            return use

        pops(first, climb(slope_two))
        tall_product(first, upstream, lambda k: w2[...], range(1), True)
        early.put(1, pltpu.matmul_pop(small[0]) + pltpu.matmul_pop(small[1]))
        pops(second, keep(o3), pieces=1)
        half = mixed_two_t.shape[0] // UNITS
        for k in range(nodes // SIDE):
            for q in range(UNITS):
                pltpu.matmul_push_rhs(upstream[span(k), :], staging_register=0, mxu_index=q)
                pltpu.matmul_acc_lhs(middle[q], mixed_two_t[q * half:(q + 1) * half, span(k)], load_staged_rhs=0)
        pops(first, keep_scaled(scaled_two))
        for q in range(UNITS):
            early.put(0, pltpu.matmul_pop(middle[q]), q * half)
        early.start_pair()
        halo_start(plan, o3, b3, hsend, hrecv, 2)
        tall_product(first, back, lambda k: scaled_two[span(k), :], order)
        tall_product(second, halo_t, lambda k: scaled_two[span(k), :], range(nodes // SIDE), pieces=1)
        early.start_spread()
        pops(first, climb(slope_one))
        product([first[q][:body] + [small_late[q]] for q in range(UNITS)],
                lambda q, i, k: mixed_t[slice(first_rows(q, i)[0], sum(first_rows(q, i))), span(k)],
                lambda k: upstream[span(k), :], range(nodes // SIDE))
        pops(second, keep(o2), pieces=1)
        for i in range(body + 1):
            for q in range(UNITS):
                late.put(0, pltpu.matmul_pop((first[q][:body] + [small_late[q]])[i]), first_rows(q, i)[0])
        late.start_pair()

    small_rows = up_to(classes, 16)
    pl.run_scoped(rest_of_step, *accs_of([SIDE] * 3 + [mixed_two_t.shape[0] // UNITS, small_rows, strip]))
    late.start_spread()
    early.start_gather()
    late.start_gather()
    halo_start(plan, o2, b2, hsend, hrecv, 3)
    early.start_back()
    early.finish()
    late.start_back()
    late.finish()
    for way, (src, dst) in enumerate(((s2, n2), (s3, n3), (o3, b3), (o2, b2))):
        halo_finish(plan, src, dst, hsend, hrecv, way)


def finish_kernel(plan, early_sizes, late_sizes, whole_early, whole_late, n2, n3, b2, b3, g1, g2, g3, m2, m3, a2, a3, h1, h2, h3, sem):
    copies = [pltpu.make_async_copy(src, dst, sem.at[i]) for i, (src, dst) in enumerate(((n2, m2), (n3, m3), (b2, a2), (b3, a3)))]
    for copy in copies:
        copy.start()
    for i, (ref, out, whole, sizes, part) in enumerate((
            (h1, g1, whole_late, late_sizes, 0), (h2, g2, whole_early, early_sizes, 0), (h3, g3, whole_early, early_sizes, 1))):
        at, chunk = slabs(sizes, plan.chips)[part]
        for core in range(plan.pair):
            for k in range(-(-ref.shape[0] // chunk)):
                rows = min(chunk, ref.shape[0] - k * chunk)
                ref[k * chunk:k * chunk + rows, core * plan.lanes:(core + 1) * plan.lanes] = whole[core, k, at:at + rows, :].astype(F32)
        copies.append(pltpu.make_async_copy(ref, out, sem.at[4 + i]))
        copies[-1].start()
    for copy in copies:
        copy.wait()


def per_device(mesh, features, local_mask, halo_mask, boundary_index, labels, halo_first, halo_second, halo_third,
               return_second, return_third, weight_first, weight_second, weight_third):
    features, local_mask, halo_mask = features[0, 0], local_mask[0, 0], halo_mask[0, 0]
    index, labels = boundary_index[0, 0], labels[0, 0]
    halo_first, halo_second, halo_third = halo_first[0, 0], halo_second[0, 0], halo_third[0, 0]
    return_second, return_third = return_second[0, 0], return_third[0, 0]
    nodes, width = features.shape
    slots, hidden, classes = index.shape[0], weight_first.shape[1], weight_third.shape[1]
    plan = Plan(mesh, hidden)
    early_sizes, late_sizes = (weight_second.shape[0], classes), (width,)
    tiles = 4 if nodes % 512 == 0 else 1
    values = (local_mask, halo_mask, features.T, halo_first.T, halo_second, halo_third, return_second, return_third,
              weight_first, weight_second, weight_third.T, index[None, :], labels[None, :])
    values = tuple(pltpu.with_memory_space_constraint(v, pltpu.HBM) for v in values)
    vmem, anywhere = pl.BlockSpec(memory_space=pltpu.VMEM), pl.BlockSpec(memory_space=pl.ANY)
    dma = pltpu.SemaphoreType.DMA
    block = jax.ShapeDtypeStruct((slots, hidden), BF)
    every = nodes + slots

    def held(value):
        return pltpu.VMEM(value.shape, value.dtype)

    done = pl.pallas_call(
        functools.partial(step_kernel, plan, tiles, early_sizes, late_sizes),
        out_shape=tuple(jax.ShapeDtypeStruct((plan.pair, plan.chips, slab_rows(sizes, plan.chips), plan.lanes), BF)
                        for sizes in (early_sizes, late_sizes)) + (block,) * 4,
        in_specs=[anywhere] * len(values), out_specs=(vmem,) * 6,
        scratch_shapes=[
            dma((len(values) + 2 * tiles,)), held(local_mask), held(halo_mask), pltpu.VMEM((width, every), BF),
            pltpu.VMEM((every, hidden), BF), pltpu.VMEM((every, hidden), BF), pltpu.VMEM((every, hidden), BF),
            pltpu.VMEM((every, hidden), BF), held(values[8]), held(values[9]), held(values[10]), held(values[11]), held(values[12]),
            pltpu.VMEM((nodes, every), BF), pltpu.VMEM((nodes, every), BF), pltpu.VMEM((slots, nodes), BF),
            pltpu.VMEM((slots, nodes), BF), pltpu.VMEM((nodes, hidden), F32), pltpu.VMEM((up_to(width, 16 * UNITS), nodes), BF),
            pltpu.VMEM((nodes, hidden), BF), pltpu.VMEM((hidden, nodes), BF), pltpu.VMEM((nodes, hidden), BF), pltpu.VMEM((nodes, hidden), F32),
            pltpu.VMEM((nodes, hidden), F32), pltpu.VMEM((nodes, hidden), BF), pltpu.VMEM((up_to(classes, 128), nodes), BF),
            pltpu.VMEM((nodes, up_to(classes, 128)), F32), pltpu.VMEM((SIDE, hidden), BF)]
        + [pltpu.VMEM((slots, hidden), BF)] * 4 + [dma((4, 4)), dma((4, 4))]
        + summer_scratch(plan, early_sizes) + summer_scratch(plan, late_sizes),
        compiler_params=pltpu.CompilerParams(collective_id=0, has_side_effects=True, vmem_limit_bytes=40 * 2**20),
        name="step",
    )(*values)
    grads = ((weight_first.shape, F32), (weight_second.shape, F32), (weight_third.shape[::-1], F32))
    out = pl.pallas_call(
        functools.partial(finish_kernel, plan, early_sizes, late_sizes),
        out_shape=tuple(jax.ShapeDtypeStruct(*g) for g in grads) + (block,) * 4,
        in_specs=[vmem] * 6, out_specs=(anywhere,) * 7,
        scratch_shapes=[pltpu.VMEM(*g) for g in grads] + [dma((7,))],
        compiler_params=pltpu.CompilerParams(vmem_limit_bytes=16 * 2**20), name="finish",
    )(*done)
    return (out[0], out[1], out[2].T) + tuple(v[None, None] for v in out[3:])


def solution(mesh):
    wide, flat, copied = P("row", "col", None, None), P("row", "col", None), P()
    return jax.shard_map(
        functools.partial(per_device, mesh), mesh=mesh,
        in_specs=(wide, wide, wide, flat, flat, wide, wide, wide, wide, wide, copied, copied, copied),
        out_specs=(copied, copied, copied, wide, wide, wide, wide),
        check_vma=False,
    )
```

```python
import functools

import jax
import jax.numpy as jnp
from jax import lax
from jax.experimental import pallas as pl
from jax.experimental.pallas import tpu as pltpu
from jax.sharding import PartitionSpec as P

MESH = pl.DeviceIdType.MESH
BF = jnp.bfloat16
F32 = jnp.float32


def up_to(value, step):
    return -(-value // step) * step


def dot(a, b, dims=((1,), (0,))):
    return lax.dot_general(a, b, (dims, ((), ())), preferred_element_type=F32)


def slope(pre, sigma):
    return sigma * (1.0 + pre * (1.0 - sigma))


class Plan:
    def __init__(self, mesh, hidden):
        self.n_row, self.n_col = mesh.shape["row"], mesh.shape["col"]
        self.pair = 2 if self.n_row % 2 == 0 else 1
        self.deep = self.n_row // self.pair
        self.chips = self.deep * self.n_col
        self.lanes = hidden // self.pair
        self.ways = range(self.chips - 1)

    def place(self):
        self.r, self.c = lax.axis_index("row"), lax.axis_index("col")
        self.core, self.z = self.r % self.pair, self.r // self.pair
        self.mate = self.r + 1 - 2 * self.core
        self.chip = self.z * self.n_col + self.c

    def peer(self, way):
        index = way + jnp.where(way >= self.chip, 1, 0)
        z, c = index // self.n_col, index % self.n_col
        return index, (z * self.pair + self.core, c), self.chip - jnp.where(way < self.chip, 1, 0)

    def greet(self):
        barrier = pltpu.get_barrier_semaphore()

        def hello(device):
            pl.semaphore_signal(barrier, inc=1, device_id=device, device_id_type=MESH)

        count = 0
        if self.pair == 2:
            hello((self.mate, self.c))
            count += 1
        for way in self.ways:
            hello(self.peer(way)[1])
            count += 1
        for step, there in self.far_rows():
            @pl.when(there)
            def _():
                hello((self.r + step, self.c))
        for _, there in self.far_rows():
            count = count + jnp.where(there, 1, 0)
        return lambda: pl.semaphore_wait(barrier, count)

    def far_rows(self):
        if self.pair == 2:
            return ((-1, jnp.logical_and(self.core == 0, self.r > 0)),
                    (1, jnp.logical_and(self.core == 1, self.r < self.n_row - 1)))
        return ()

    def turns(self):
        return ((3, 1, 3, 2, 2), (2, 2, 0, 1, 3)) if self.n_col == 4 else ()

    def edges(self):
        r, c = self.r, self.c
        return (((r - 1, c), 1, r > 0), ((r + 1, c), 0, r < self.n_row - 1),
                ((r, c - 1), 3, c > 0), ((r, c + 1), 2, c < self.n_col - 1))


def halo_copy(plan, k, src, dst, send, recv, way):
    bound = src.shape[0] // 4
    device, slot, there = plan.edges()[k]
    copy = pltpu.make_async_remote_copy(
        src_ref=src.at[pl.ds(k * bound, bound)], dst_ref=dst.at[pl.ds(slot * bound, bound)],
        send_sem=send.at[way, k], recv_sem=recv.at[way, slot], device_id=device, device_id_type=MESH)
    return copy, slot, there


def halo_start(plan, src, dst, send, recv, way, relay=None):
    bound = src.shape[0] // 4
    for k in range(4):
        copy, _, there = halo_copy(plan, k, src, dst, send, recv, way)
        turns = [turn for turn in plan.turns() if relay is not None and turn[0] == k]
        for _, origin, middle, _, _ in turns:
            there = jnp.logical_and(there, plan.c != origin)

            @pl.when(plan.c == origin)
            def _():
                pltpu.make_async_remote_copy(
                    src_ref=src.at[pl.ds(k * bound, bound)], dst_ref=relay[0].at[way], send_sem=send.at[way, k],
                    recv_sem=relay[2].at[way], device_id=(plan.r, middle), device_id_type=MESH).start()

        @pl.when(there)
        def _():
            copy.start()


def relay_copy(plan, turn, dst, recv, way, relay):
    bound = dst.shape[0] // 4
    return pltpu.make_async_remote_copy(
        src_ref=relay[0].at[way], dst_ref=dst.at[pl.ds(turn[4] * bound, bound)], send_sem=relay[1].at[way],
        recv_sem=recv.at[way, turn[4]], device_id=(plan.r, turn[3]), device_id_type=MESH)


def relay_start(plan, dst, recv, way, relay):
    for turn in plan.turns():
        @pl.when(plan.c == turn[2])
        def _():
            pltpu.make_async_remote_copy(
                src_ref=relay[0].at[way], dst_ref=relay[0].at[way], send_sem=relay[1].at[way],
                recv_sem=relay[2].at[way], device_id=(plan.r, turn[1]), device_id_type=MESH).wait_recv()
            relay_copy(plan, turn, dst, recv, way, relay).start()


def relay_finish(plan, dst, recv, way, relay):
    for turn in plan.turns():
        @pl.when(plan.c == turn[2])
        def _():
            relay_copy(plan, turn, dst, recv, way, relay).wait_send()


def halo_clear(plan, dsts):
    bound = dsts[0].shape[0] // 4
    for k in range(4):
        @pl.when(jnp.logical_not(plan.edges()[k][2]))
        def _():
            for dst in dsts:
                dst[pl.ds(k * bound, bound), :] = jnp.zeros((bound, dst.shape[1]), dst.dtype)


def halo_finish(plan, src, dst, send, recv, way):
    bound = src.shape[0] // 4
    for k in range(4):
        copy, _, there = halo_copy(plan, k, src, dst, send, recv, way)
        arrival = pltpu.make_async_remote_copy(
            src_ref=src.at[pl.ds(k * bound, bound)], dst_ref=dst.at[pl.ds(k * bound, bound)],
            send_sem=send.at[way, k], recv_sem=recv.at[way, k], device_id=plan.edges()[k][0], device_id_type=MESH)

        @pl.when(there)
        def _():
            copy.wait_send()
            arrival.wait_recv()


class Summer:
    def __init__(self, plan, sizes, own, mine, got_pair, acc, got, whole, sems):
        self.plan, self.sizes, self.own, self.mine, self.got_pair = plan, sizes, own, mine, got_pair
        self.acc, self.got, self.whole, self.sems = acc, got, whole, sems

    def copy(self, src, dst, kind, d, device, there=None):
        return pltpu.make_async_remote_copy(
            src_ref=src, dst_ref=dst, send_sem=self.sems[2 * kind].at[d],
            recv_sem=self.sems[2 * kind + 1].at[d if there is None else there],
            device_id=device, device_id_type=MESH)

    def clear(self):
        self.own[...] = jnp.zeros_like(self.own)
        self.mine[...] = jnp.zeros_like(self.mine)

    def put(self, i, value, row=0):
        at, chunk = slabs(self.sizes, self.plan.chips)[i]
        end = min(row + value.shape[0], self.sizes[i])
        for k in range(row // chunk, -(-end // chunk)):
            low, high = max(row, k * chunk), min(end, (k + 1) * chunk)
            for core in range(self.plan.pair):
                part = value[low - row:high - row, core * self.plan.lanes:(core + 1) * self.plan.lanes]
                place = slice(at + low - k * chunk, at + high - k * chunk)
                self.own[core, k, place, :] = part
                self.mine[core, k, place, :] = part.astype(BF)

    def pair_copy(self):
        return self.copy(self.mine.at[1 - self.plan.core], self.got_pair, 0, 0, (self.plan.mate, self.plan.c))

    def start_pair(self):
        if self.plan.pair == 2:
            self.pair_copy().start()

    def spread_copy(self, d):
        index, device, there = self.plan.peer(d)
        return self.copy(self.acc.at[index], self.got.at[there], 1, d, device, there)

    def start_spread(self):
        if self.plan.pair == 2:
            self.pair_copy().wait()
            self.acc[...] = (self.own[self.plan.core] + self.got_pair[...].astype(F32)).astype(BF)
        else:
            self.acc[...] = self.mine[0]
        for d in self.plan.ways:
            self.spread_copy(d).start()

    def gather_copy(self, d):
        _, device, there = self.plan.peer(d)
        part = self.whole.at[self.plan.core, self.plan.chip]
        return self.copy(part, part, 2, d, device, there)

    def back_copy(self, d, core):
        index = self.plan.chip if d == len(self.plan.ways) else self.plan.peer(d)[0]
        part = self.whole.at[core, index]
        return self.copy(part, part, 3, d, (self.plan.mate, self.plan.c))

    def start_gather(self):
        plan = self.plan
        total = self.own[plan.core, plan.chip]
        if plan.pair == 2:
            total = total + self.got_pair[plan.chip].astype(F32)
        for d in plan.ways:
            index, device, _ = plan.peer(d)
            self.spread_copy(d).wait_send()
            self.copy(self.acc.at[index], self.got.at[d], 1, d, device).wait_recv()
            total = total + self.got[d].astype(F32)
        self.whole[plan.core, plan.chip] = total.astype(BF)
        for d in plan.ways:
            self.gather_copy(d).start()
        if plan.pair == 2:
            self.back_copy(len(plan.ways), plan.core).start()

    def start_back(self):
        plan = self.plan
        for d in plan.ways:
            index, device, _ = plan.peer(d)
            part = self.whole.at[plan.core, index]
            self.copy(part, part, 2, d, device).wait_recv()
            if plan.pair == 2:
                self.back_copy(d, plan.core).start()

    def finish(self):
        plan = self.plan
        for d in plan.ways:
            self.gather_copy(d).wait_send()
        if plan.pair == 2:
            for d in range(len(plan.ways) + 1):
                self.back_copy(d, plan.core).wait_send()
                self.back_copy(d, 1 - plan.core).wait_recv()


def slabs(sizes, chips):
    out, at = [], 0
    for size in sizes:
        chunk = up_to(-(-size // chips), 8)
        out.append((at, chunk))
        at += chunk
    return out


def slab_rows(sizes, chips):
    return sum(chunk for _, chunk in slabs(sizes, chips))


def summer_scratch(plan, sizes):
    rows, dma, n = slab_rows(sizes, plan.chips), pltpu.SemaphoreType.DMA, max(len(plan.ways), 1)
    full = (plan.chips, rows, plan.lanes)
    return [pltpu.VMEM((plan.pair,) + full, F32), pltpu.VMEM((plan.pair,) + full, BF), pltpu.VMEM(full, BF),
            pltpu.VMEM(full, BF), pltpu.VMEM((n, rows, plan.lanes), BF),
            dma((1,)), dma((1,)), dma((n,)), dma((n,)), dma((n,)), dma((n,)), dma((n + 1,)), dma((n + 1,))]


SUMMER_REFS = 13
LATE_AT = 1
UNITS, SIDE = 2, 256


NAMES = ("local", "halo", "features", "halo_first", "halo_second", "halo_third", "return_second", "return_third",
         "weight_first", "weight_second", "weight_third", "index_row", "labels")


def product(accs, lhs, rhs, depth, transpose=False):
    for k in depth:
        for q in range(UNITS):
            pltpu.matmul_push_rhs(rhs(k), staging_register=0, mxu_index=q, transpose=transpose)
            for i, acc in enumerate(accs[q]):
                pltpu.matmul_acc_lhs(acc, lhs(q, i, k), load_staged_rhs=0 if i == 0 else None)


def padded(value, rows, lanes=None):
    if value.shape[0] < rows:
        value = jnp.concatenate([value, jnp.zeros((rows - value.shape[0], value.shape[1]), value.dtype)], axis=0)
    if lanes is not None and value.shape[1] < lanes:
        value = jnp.concatenate([value, jnp.zeros((value.shape[0], lanes - value.shape[1]), value.dtype)], axis=1)
    return value


def span(k):
    return slice(k * SIDE, (k + 1) * SIDE)


def step_kernel(plan, tiles, early_sizes, late_sizes, *refs):
    count = len(NAMES)
    hbm = dict(zip(NAMES, refs[:count]))
    whole_early, whole_late, n2, n3, b2, b3 = refs[count:count + 6]
    (in_sem, local_i, halo_i, x_t, values_two, values_three, scaled_three, scaled_two, w1, w2, w3, index_row, labels,
     near_far, back, halo_t, hits_t, inverse, mixed_t, mixed_two, mixed_two_t, mixed_three, slope_one, slope_two, upstream,
     upstream_three_t, target_held, w3_wide, s2, s3, o2, o3, hsend, hrecv, *relay) = refs[count + 6:count + 43]
    rest = refs[count + 43:]
    early, late = (Summer(plan, sizes, *part[:5], whole, part[5:]) for sizes, part, whole in (
        (early_sizes, rest[:SUMMER_REFS], whole_early), (late_sizes, rest[SUMMER_REFS:], whole_late)))
    nodes, slots = local_i.shape[0], halo_i.shape[1]
    every, width, classes = nodes + slots, x_t.shape[0], w3.shape[0]
    plan.place()

    own, other = pl.ds(0, nodes), pl.ds(nodes, slots)
    tall = nodes // tiles
    tile = [slice(t * tall, (t + 1) * tall) for t in range(tiles)]
    targets = {"features": (x_t, 1, 0), "halo_first": (x_t, 1, nodes), "halo_second": (values_two, 0, nodes),
               "halo_third": (values_three, 0, nodes), "return_second": (scaled_two, 0, nodes),
               "return_third": (scaled_three, 0, nodes), "weight_first": (w1, 0, 0), "weight_second": (w2, 0, 0),
               "weight_third": (w3, 0, 0), "index_row": (index_row, 0, 0), "labels": (labels, 0, 0)}
    slot = {}

    class Load:
        def __init__(self, key):
            self.key = key

        def copy(self):
            index = slot.setdefault(self.key, len(slot))
            if isinstance(self.key, tuple):
                name, t = self.key
                rows = pl.ds(t * tall, tall)
                return pltpu.make_async_copy(hbm[name].at[rows], {"local": local_i, "halo": halo_i}[name].at[rows], in_sem.at[index])
            ref, axis, start = targets[self.key]
            part = pl.ds(start, hbm[self.key].shape[axis])
            return pltpu.make_async_copy(hbm[self.key], ref.at[:, part] if axis else ref.at[part], in_sem.at[index])

        def start(self):
            self.copy().start()

        def wait(self):
            self.copy().wait()

    loads = {}

    def load(key):
        loads[key] = Load(key)
        loads[key].start()

    late_names = ("halo_second", "halo_third", "return_third", "return_second", "weight_third")

    def load_tile(t):
        load(("local", t))
        load(("halo", t))

    def load_named(names):
        for name in names:
            load(name)

    load_tile(0)
    first_names = ("features", "halo_first", "weight_first", "index_row", "labels", "weight_second")
    load_named(first_names)
    for t in range(1, tiles):
        load_tile(t)

    halo_clear(plan, (n2, n3, b2, b3))
    met = plan.greet()
    early.clear()
    late.clear()
    wide = target_held.shape[1]

    def mark():
        back[:, other] = jnp.where(lax.broadcasted_iota(jnp.int32, (nodes, slots), 0) == index_row[...], 1.0, 0.0).astype(BF)
        hits_t[...] = back[:, other].T
        target_held[...] = jnp.where(lax.broadcasted_iota(jnp.int32, (wide, nodes), 0) == labels[...], 1.0, 0.0).T
        w3_wide[...] = jnp.zeros_like(w3_wide)

    tail = up_to(width, 16 * UNITS) - UNITS * SIDE * (width // (UNITS * SIDE))
    body = width // (UNITS * SIDE)
    strip = tail // UNITS

    def first_rows(q, i):
        return ((q + UNITS * i) * SIDE, SIDE) if i < body else (UNITS * SIDE * body + q * strip, strip)

    def first_layer(*accs):
        mix = [[accs[q + UNITS * (i + (body + 1) * b)] for q in range(UNITS) for i in range(body + 1)] for b in range(2)]
        mix = [[m[q * (body + 1):(q + 1) * (body + 1)] for q in range(UNITS)] for m in mix]
        pres = accs[2 * UNITS * (body + 1):]
        for acc in accs:
            pltpu.matmul_pop(acc)

        def gather(t):
            loads[("local", t)].wait()
            loads[("halo", t)].wait()
            if t == LATE_AT:
                load_named(late_names)
            if t == tiles - 1:
                loads[late_names[0]].wait()
            near, far = local_i[tile[t], :].astype(F32), halo_i[tile[t], :].astype(F32)
            total = 1.0 + jnp.sum(near, axis=1, keepdims=True) + jnp.sum(far, axis=1, keepdims=True)
            near_far[tile[t], own] = near.astype(BF)
            near_far[tile[t], other] = far.astype(BF)
            square = near[:, tile[t]]
            here = lax.broadcasted_iota(jnp.int32, square.shape, 0) == lax.broadcasted_iota(jnp.int32, square.shape, 1)
            near_far[tile[t], tile[t]] = jnp.where(here, square + 1.0, square).astype(BF)
            inverse[tile[t], :] = jnp.broadcast_to(1.0 / total, (tall, inverse.shape[1]))

        def mix_tile(t):
            product(mix[t % 2], lambda q, i, k: padded(x_t[slice(first_rows(q, i)[0], min(sum(first_rows(q, i)), width)), span(k)], first_rows(q, i)[1]),
                    lambda k: near_far[tile[t], span(k)], range(every // SIDE), True)

        def settle(t):
            pre_acc = [pres[UNITS * (t % 2) + q] for q in range(UNITS)]
            half = tall // UNITS
            across = inverse[tile[t], :128].T[0:1]
            for i in range(body + 1):
                for q in range(UNITS):
                    start, size = first_rows(q, i)
                    mixed_t[start:start + size, tile[t]] = (pltpu.matmul_pop(mix[t % 2][q][i]) * across).astype(BF)
            back[own, tile[t]] = near_far[tile[t], own].T
            halo_t[:, tile[t]] = near_far[tile[t], other].T
            depth = -(-width // SIDE)
            turned = [mixed_t[k * SIDE:min((k + 1) * SIDE, mixed_t.shape[0]), tile[t]].T for k in range(depth)]
            product([[acc] for acc in pre_acc], lambda q, i, k: padded(turned[k][q * half:(q + 1) * half], half, SIDE),
                    lambda k: padded(w1[k * SIDE:min((k + 1) * SIDE, width), :], SIDE), range(depth))

        def close(t):
            half = tall // UNITS
            for q in range(UNITS):
                rows = slice(t * tall + q * half, t * tall + (q + 1) * half)
                pre = pltpu.matmul_pop(pres[UNITS * (t % 2) + q])
                sigma = jax.nn.sigmoid(pre)
                values_two[rows, :] = (pre * sigma).astype(BF)
                slope_one[rows, :] = slope(pre, sigma)

        for t in range(tiles):
            gather(t)
            if t == 0:
                for name in first_names:
                    loads[name].wait()
            mix_tile(t)
            if t == 0:
                mark()
            if t > 1:
                close(t - 2)
            if t > 0:
                settle(t - 1)
        if tiles > 1:
            close(tiles - 2)
        settle(tiles - 1)
        close(tiles - 1)

    def accs_of(sizes):
        return [pltpu.ACC(q)((size, SIDE), F32) for size in sizes for q in range(UNITS)]

    sizes = ([SIDE] * body + [strip]) * 2 + [tall // UNITS] * 2
    pl.run_scoped(first_layer, *accs_of(sizes))

    order = list(range(nodes // SIDE, every // SIDE)) + list(range(nodes // SIDE))

    def rest_of_step(*accs):
        held = [[accs[q + UNITS * i] for i in range(6)] for q in range(UNITS)]
        first, second = [p[0:2] for p in held], [p[2:3] for p in held]
        middle, small, small_late = ([p[i] for p in held] for i in (3, 4, 5))

        def at(q, i):
            return slice((q + UNITS * i) * SIDE, (q + UNITS * i + 1) * SIDE)

        def tall_product(sets, left, right, depth, transpose=False, pieces=2):
            for i in range(pieces):
                product([[sets[q][i]] for q in range(UNITS)], lambda q, _, k: left[at(q, i), span(k)],
                        lambda k: right(k), depth, transpose)

        def pops(sets, use, pieces=2):
            for i in range(pieces):
                for q in range(UNITS):
                    use(at(q, i), pltpu.matmul_pop(sets[q][i]))

        def keep_mixed(mixed, mixed_turned):
            def use(rows, value):
                out = (value * inverse[rows, :]).astype(BF)
                mixed[rows, :] = out
                if mixed_turned is not None:
                    mixed_turned[:, rows] = out.T
            return use

        def keep(out):
            def use(rows, value):
                out[rows, :] = value.astype(BF)
            return use

        def keep_scaled(out):
            def use(rows, value):
                out[rows, :] = (value * inverse[rows, :]).astype(BF)
            return use

        tall_product(first, near_far, lambda k: values_two[span(k), :], order)
        tall_product(second, hits_t, lambda k: values_two[span(k), :], range(nodes // SIDE), pieces=1)
        pops(first, keep_mixed(mixed_two, mixed_two_t))
        tall_product(first, mixed_two, lambda k: w2[...], range(1))
        pops(second, keep(s2), pieces=1)

        def activate(rows, pre):
            sigma = jax.nn.sigmoid(pre)
            values_three[rows, :] = (pre * sigma).astype(BF)
            slope_two[rows, :] = slope(pre, sigma)

        pops(first, activate)
        for name in late_names[1:]:
            loads[name].wait()
        w3_wide[0:classes, :] = w3[...]
        met()
        halo_start(plan, s2, n2, hsend, hrecv, 0, relay)
        tall_product(first, near_far, lambda k: values_three[span(k), :], order)
        tall_product(second, hits_t, lambda k: values_three[span(k), :], range(nodes // SIDE), pieces=1)
        pops(first, keep_mixed(mixed_three, None))
        tall_product(first, mixed_three, lambda k: w3_wide[...], range(1), True)
        pops(second, keep(s3), pieces=1)
        ups = {}

        def soften(rows, logits):
            logits = logits[:, :wide]
            inside = lax.broadcasted_iota(jnp.int32, logits.shape, 1) < classes
            expo = jnp.where(inside, jnp.exp(logits), 0.0)
            probs = expo / jnp.sum(expo, axis=1, keepdims=True)
            up = ((probs - target_held[rows, :]) / nodes).astype(BF)
            upstream_three_t[:, rows] = up.T
            ups[rows.start] = padded(up, up.shape[0], SIDE)

        pops(first, soften)
        for i in range(2):
            product([[first[q][i]] for q in range(UNITS)], lambda q, _, k: ups[at(q, i).start], lambda k: w3_wide[...], range(1))
        pops(first, keep_scaled(scaled_three))
        halo_start(plan, s3, n3, hsend, hrecv, 1, relay)
        tall_product(first, back, lambda k: scaled_three[span(k), :], order)
        stripes = nodes // SIDE // UNITS
        for k in range(stripes):
            for q in range(UNITS):
                pltpu.matmul_push_rhs(mixed_three[span(q * stripes + k), :], staging_register=0, mxu_index=q)
                pltpu.matmul_acc_lhs(small[q], upstream_three_t[0:small_rows, span(q * stripes + k)], load_staged_rhs=0)
        tall_product(second, halo_t, lambda k: scaled_three[span(k), :], range(nodes // SIDE), pieces=1)

        def climb(slopes):
            def use(rows, value):
                upstream[rows, :] = (value * slopes[rows, :]).astype(BF)
            return use

        pops(first, climb(slope_two))
        tall_product(first, upstream, lambda k: w2[...], range(1), True)
        early.put(1, pltpu.matmul_pop(small[0]) + pltpu.matmul_pop(small[1]))
        pops(second, keep(o3), pieces=1)
        half = mixed_two_t.shape[0] // UNITS
        for k in range(nodes // SIDE):
            for q in range(UNITS):
                pltpu.matmul_push_rhs(upstream[span(k), :], staging_register=0, mxu_index=q)
                pltpu.matmul_acc_lhs(middle[q], mixed_two_t[q * half:(q + 1) * half, span(k)], load_staged_rhs=0)
        pops(first, keep_scaled(scaled_two))
        for q in range(UNITS):
            early.put(0, pltpu.matmul_pop(middle[q]), q * half)
        early.start_pair()
        relay_start(plan, n2, hrecv, 0, relay)
        halo_start(plan, o3, b3, hsend, hrecv, 2)
        tall_product(first, back, lambda k: scaled_two[span(k), :], order)
        tall_product(second, halo_t, lambda k: scaled_two[span(k), :], range(nodes // SIDE), pieces=1)
        early.start_spread()
        pops(first, climb(slope_one))
        product([first[q][:body] + [small_late[q]] for q in range(UNITS)],
                lambda q, i, k: mixed_t[slice(first_rows(q, i)[0], sum(first_rows(q, i))), span(k)],
                lambda k: upstream[span(k), :], range(nodes // SIDE))
        pops(second, keep(o2), pieces=1)
        for i in range(body + 1):
            for q in range(UNITS):
                late.put(0, pltpu.matmul_pop((first[q][:body] + [small_late[q]])[i]), first_rows(q, i)[0])
        late.start_pair()

    small_rows = up_to(classes, 16)
    pl.run_scoped(rest_of_step, *accs_of([SIDE] * 3 + [mixed_two_t.shape[0] // UNITS, small_rows, strip]))
    late.start_spread()
    relay_start(plan, n3, hrecv, 1, relay)
    early.start_gather()
    late.start_gather()
    halo_start(plan, o2, b2, hsend, hrecv, 3)
    early.start_back()
    early.finish()
    late.start_back()
    late.finish()
    relay_finish(plan, n2, hrecv, 0, relay)
    relay_finish(plan, n3, hrecv, 1, relay)
    for way, (src, dst) in enumerate(((s2, n2), (s3, n3), (o3, b3), (o2, b2))):
        halo_finish(plan, src, dst, hsend, hrecv, way)


def finish_kernel(plan, early_sizes, late_sizes, whole_early, whole_late, n2, n3, b2, b3, g1, g2, g3, m2, m3, a2, a3, h1, h2, h3, sem):
    copies = [pltpu.make_async_copy(src, dst, sem.at[i]) for i, (src, dst) in enumerate(((n2, m2), (n3, m3), (b2, a2), (b3, a3)))]
    for copy in copies:
        copy.start()
    for i, (ref, out, whole, sizes, part) in enumerate((
            (h1, g1, whole_late, late_sizes, 0), (h2, g2, whole_early, early_sizes, 0), (h3, g3, whole_early, early_sizes, 1))):
        at, chunk = slabs(sizes, plan.chips)[part]
        for core in range(plan.pair):
            for k in range(-(-ref.shape[0] // chunk)):
                rows = min(chunk, ref.shape[0] - k * chunk)
                ref[k * chunk:k * chunk + rows, core * plan.lanes:(core + 1) * plan.lanes] = whole[core, k, at:at + rows, :].astype(F32)
        copies.append(pltpu.make_async_copy(ref, out, sem.at[4 + i]))
        copies[-1].start()
    for copy in copies:
        copy.wait()


def per_device(mesh, features, local_mask, halo_mask, boundary_index, labels, halo_first, halo_second, halo_third,
               return_second, return_third, weight_first, weight_second, weight_third):
    features, local_mask, halo_mask = features[0, 0], local_mask[0, 0], halo_mask[0, 0]
    index, labels = boundary_index[0, 0], labels[0, 0]
    halo_first, halo_second, halo_third = halo_first[0, 0], halo_second[0, 0], halo_third[0, 0]
    return_second, return_third = return_second[0, 0], return_third[0, 0]
    nodes, width = features.shape
    slots, hidden, classes = index.shape[0], weight_first.shape[1], weight_third.shape[1]
    plan = Plan(mesh, hidden)
    early_sizes, late_sizes = (weight_second.shape[0], classes), (width,)
    tiles = 4 if nodes % 512 == 0 else 1
    values = (local_mask, halo_mask, features.T, halo_first.T, halo_second, halo_third, return_second, return_third,
              weight_first, weight_second, weight_third.T, index[None, :], labels[None, :])
    values = tuple(pltpu.with_memory_space_constraint(v, pltpu.HBM) for v in values)
    vmem, anywhere = pl.BlockSpec(memory_space=pltpu.VMEM), pl.BlockSpec(memory_space=pl.ANY)
    dma = pltpu.SemaphoreType.DMA
    block = jax.ShapeDtypeStruct((slots, hidden), BF)
    every = nodes + slots

    def held(value):
        return pltpu.VMEM(value.shape, value.dtype)

    done = pl.pallas_call(
        functools.partial(step_kernel, plan, tiles, early_sizes, late_sizes),
        out_shape=tuple(jax.ShapeDtypeStruct((plan.pair, plan.chips, slab_rows(sizes, plan.chips), plan.lanes), BF)
                        for sizes in (early_sizes, late_sizes)) + (block,) * 4,
        in_specs=[anywhere] * len(values), out_specs=(vmem,) * 6,
        scratch_shapes=[
            dma((len(values) + 2 * tiles,)), held(local_mask), held(halo_mask), pltpu.VMEM((width, every), BF),
            pltpu.VMEM((every, hidden), BF), pltpu.VMEM((every, hidden), BF), pltpu.VMEM((every, hidden), BF),
            pltpu.VMEM((every, hidden), BF), held(values[8]), held(values[9]), held(values[10]), held(values[11]), held(values[12]),
            pltpu.VMEM((nodes, every), BF), pltpu.VMEM((nodes, every), BF), pltpu.VMEM((slots, nodes), BF),
            pltpu.VMEM((slots, nodes), BF), pltpu.VMEM((nodes, hidden), F32), pltpu.VMEM((up_to(width, 16 * UNITS), nodes), BF),
            pltpu.VMEM((nodes, hidden), BF), pltpu.VMEM((hidden, nodes), BF), pltpu.VMEM((nodes, hidden), BF), pltpu.VMEM((nodes, hidden), F32),
            pltpu.VMEM((nodes, hidden), F32), pltpu.VMEM((nodes, hidden), BF), pltpu.VMEM((up_to(classes, 128), nodes), BF),
            pltpu.VMEM((nodes, up_to(classes, 128)), F32), pltpu.VMEM((SIDE, hidden), BF)]
        + [pltpu.VMEM((slots, hidden), BF)] * 4 + [dma((4, 4)), dma((4, 4)), pltpu.VMEM((2, slots // 4, hidden), BF), dma((2,)), dma((2,))]
        + summer_scratch(plan, early_sizes) + summer_scratch(plan, late_sizes),
        compiler_params=pltpu.CompilerParams(collective_id=0, has_side_effects=True, vmem_limit_bytes=40 * 2**20),
        name="step",
    )(*values)
    grads = ((weight_first.shape, F32), (weight_second.shape, F32), (weight_third.shape[::-1], F32))
    out = pl.pallas_call(
        functools.partial(finish_kernel, plan, early_sizes, late_sizes),
        out_shape=tuple(jax.ShapeDtypeStruct(*g) for g in grads) + (block,) * 4,
        in_specs=[vmem] * 6, out_specs=(anywhere,) * 7,
        scratch_shapes=[pltpu.VMEM(*g) for g in grads] + [dma((7,))],
        compiler_params=pltpu.CompilerParams(vmem_limit_bytes=16 * 2**20), name="finish",
    )(*done)
    return (out[0], out[1], out[2].T) + tuple(v[None, None] for v in out[3:])


def solution(mesh):
    wide, flat, copied = P("row", "col", None, None), P("row", "col", None), P()
    return jax.shard_map(
        functools.partial(per_device, mesh), mesh=mesh,
        in_specs=(wide, wide, wide, flat, flat, wide, wide, wide, wide, wide, copied, copied, copied),
        out_specs=(copied, copied, copied, wide, wide, wide, wide),
        check_vma=False,
    )
```

```python
import functools

import jax
import jax.numpy as jnp
from jax import lax
from jax.experimental import pallas as pl
from jax.experimental.pallas import tpu as pltpu
from jax.sharding import PartitionSpec as P

MESH = pl.DeviceIdType.MESH
BF = jnp.bfloat16
F32 = jnp.float32


def up_to(value, step):
    return -(-value // step) * step


def dot(a, b, dims=((1,), (0,))):
    return lax.dot_general(a, b, (dims, ((), ())), preferred_element_type=F32)


def slope(pre, sigma):
    return sigma * (1.0 + pre * (1.0 - sigma))


class Plan:
    def __init__(self, mesh, hidden):
        self.n_row, self.n_col = mesh.shape["row"], mesh.shape["col"]
        self.pair = 2 if self.n_row % 2 == 0 else 1
        self.deep = self.n_row // self.pair
        self.chips = self.deep * self.n_col
        self.lanes = hidden // self.pair
        self.ways = range(self.chips - 1)

    def place(self):
        self.r, self.c = lax.axis_index("row"), lax.axis_index("col")
        self.core, self.z = self.r % self.pair, self.r // self.pair
        self.mate = self.r + 1 - 2 * self.core
        self.chip = self.z * self.n_col + self.c

    def peer(self, way):
        index = way + jnp.where(way >= self.chip, 1, 0)
        z, c = index // self.n_col, index % self.n_col
        return index, (z * self.pair + self.core, c), self.chip - jnp.where(way < self.chip, 1, 0)

    def greet(self):
        barrier = pltpu.get_barrier_semaphore()

        def hello(device):
            pl.semaphore_signal(barrier, inc=1, device_id=device, device_id_type=MESH)

        count = 0
        if self.pair == 2:
            hello((self.mate, self.c))
            count += 1
        for way in self.ways:
            hello(self.peer(way)[1])
            count += 1
        for step, there in self.far_rows():
            @pl.when(there)
            def _():
                hello((self.r + step, self.c))
        for _, there in self.far_rows():
            count = count + jnp.where(there, 1, 0)
        return lambda: pl.semaphore_wait(barrier, count)

    def far_rows(self):
        if self.pair == 2:
            return ((-1, jnp.logical_and(self.core == 0, self.r > 0)),
                    (1, jnp.logical_and(self.core == 1, self.r < self.n_row - 1)))
        return ()

    def turns(self):
        return ((3, 1, 3, 2, 2), (2, 2, 0, 1, 3)) if self.n_col == 4 else ()

    def edges(self):
        r, c = self.r, self.c
        return (((r - 1, c), 1, r > 0), ((r + 1, c), 0, r < self.n_row - 1),
                ((r, c - 1), 3, c > 0), ((r, c + 1), 2, c < self.n_col - 1))


def halo_copy(plan, k, src, dst, send, recv, way):
    bound = src.shape[0] // 4
    device, slot, there = plan.edges()[k]
    copy = pltpu.make_async_remote_copy(
        src_ref=src.at[pl.ds(k * bound, bound)], dst_ref=dst.at[pl.ds(slot * bound, bound)],
        send_sem=send.at[way, k], recv_sem=recv.at[way, slot], device_id=device, device_id_type=MESH)
    return copy, slot, there


def halo_start(plan, src, dst, send, recv, way, relay=None):
    bound = src.shape[0] // 4
    for k in range(4):
        copy, _, there = halo_copy(plan, k, src, dst, send, recv, way)
        turns = [turn for turn in plan.turns() if relay is not None and turn[0] == k]
        for _, origin, middle, _, _ in turns:
            there = jnp.logical_and(there, plan.c != origin)

            @pl.when(plan.c == origin)
            def _():
                pltpu.make_async_remote_copy(
                    src_ref=src.at[pl.ds(k * bound, bound)], dst_ref=relay[0].at[way], send_sem=send.at[way, k],
                    recv_sem=relay[2].at[way], device_id=(plan.r, middle), device_id_type=MESH).start()

        @pl.when(there)
        def _():
            copy.start()


def relay_copy(plan, turn, dst, recv, way, relay):
    bound = dst.shape[0] // 4
    return pltpu.make_async_remote_copy(
        src_ref=relay[0].at[way], dst_ref=dst.at[pl.ds(turn[4] * bound, bound)], send_sem=relay[1].at[way],
        recv_sem=recv.at[way, turn[4]], device_id=(plan.r, turn[3]), device_id_type=MESH)


def relay_start(plan, dst, recv, way, relay):
    for turn in plan.turns():
        @pl.when(plan.c == turn[2])
        def _():
            pltpu.make_async_remote_copy(
                src_ref=relay[0].at[way], dst_ref=relay[0].at[way], send_sem=relay[1].at[way],
                recv_sem=relay[2].at[way], device_id=(plan.r, turn[1]), device_id_type=MESH).wait_recv()
            relay_copy(plan, turn, dst, recv, way, relay).start()


def relay_finish(plan, dst, recv, way, relay):
    for turn in plan.turns():
        @pl.when(plan.c == turn[2])
        def _():
            relay_copy(plan, turn, dst, recv, way, relay).wait_send()


def halo_clear(plan, dsts):
    bound = dsts[0].shape[0] // 4
    for k in range(4):
        @pl.when(jnp.logical_not(plan.edges()[k][2]))
        def _():
            for dst in dsts:
                dst[pl.ds(k * bound, bound), :] = jnp.zeros((bound, dst.shape[1]), dst.dtype)


def halo_finish(plan, src, dst, send, recv, way):
    bound = src.shape[0] // 4
    for k in range(4):
        copy, _, there = halo_copy(plan, k, src, dst, send, recv, way)
        arrival = pltpu.make_async_remote_copy(
            src_ref=src.at[pl.ds(k * bound, bound)], dst_ref=dst.at[pl.ds(k * bound, bound)],
            send_sem=send.at[way, k], recv_sem=recv.at[way, k], device_id=plan.edges()[k][0], device_id_type=MESH)

        @pl.when(there)
        def _():
            copy.wait_send()
            arrival.wait_recv()


class Summer:
    def __init__(self, plan, sizes, own, mine, got_pair, acc, got, whole, sems):
        self.plan, self.sizes, self.own, self.mine, self.got_pair = plan, sizes, own, mine, got_pair
        self.acc, self.got, self.whole, self.sems = acc, got, whole, sems

    def copy(self, src, dst, kind, d, device, there=None):
        return pltpu.make_async_remote_copy(
            src_ref=src, dst_ref=dst, send_sem=self.sems[2 * kind].at[d],
            recv_sem=self.sems[2 * kind + 1].at[d if there is None else there],
            device_id=device, device_id_type=MESH)

    def clear(self):
        self.own[...] = jnp.zeros_like(self.own)
        self.mine[...] = jnp.zeros_like(self.mine)

    def put(self, i, value, row=0):
        at, chunk = slabs(self.sizes, self.plan.chips)[i]
        end = min(row + value.shape[0], self.sizes[i])
        for k in range(row // chunk, -(-end // chunk)):
            low, high = max(row, k * chunk), min(end, (k + 1) * chunk)
            for core in range(self.plan.pair):
                part = value[low - row:high - row, core * self.plan.lanes:(core + 1) * self.plan.lanes]
                place = slice(at + low - k * chunk, at + high - k * chunk)
                self.own[core, k, place, :] = part
                self.mine[core, k, place, :] = part.astype(BF)

    def pair_copy(self):
        return self.copy(self.mine.at[1 - self.plan.core], self.got_pair, 0, 0, (self.plan.mate, self.plan.c))

    def start_pair(self):
        if self.plan.pair == 2:
            self.pair_copy().start()

    def spread_copy(self, d):
        index, device, there = self.plan.peer(d)
        return self.copy(self.acc.at[index], self.got.at[there], 1, d, device, there)

    def start_spread(self):
        if self.plan.pair == 2:
            self.pair_copy().wait()
            self.acc[...] = (self.own[self.plan.core] + self.got_pair[...].astype(F32)).astype(BF)
        else:
            self.acc[...] = self.mine[0]
        for d in self.plan.ways:
            self.spread_copy(d).start()

    def gather_copy(self, d):
        _, device, there = self.plan.peer(d)
        part = self.whole.at[self.plan.core, self.plan.chip]
        return self.copy(part, part, 2, d, device, there)

    def back_copy(self, d, core):
        index = self.plan.chip if d == len(self.plan.ways) else self.plan.peer(d)[0]
        part = self.whole.at[core, index]
        return self.copy(part, part, 3, d, (self.plan.mate, self.plan.c))

    def start_gather(self):
        plan = self.plan
        total = self.own[plan.core, plan.chip]
        if plan.pair == 2:
            total = total + self.got_pair[plan.chip].astype(F32)
        for d in plan.ways:
            index, device, _ = plan.peer(d)
            self.spread_copy(d).wait_send()
            self.copy(self.acc.at[index], self.got.at[d], 1, d, device).wait_recv()
            total = total + self.got[d].astype(F32)
        self.whole[plan.core, plan.chip] = total.astype(BF)
        for d in plan.ways:
            self.gather_copy(d).start()
        if plan.pair == 2:
            self.back_copy(len(plan.ways), plan.core).start()

    def start_back(self):
        plan = self.plan
        for d in plan.ways:
            index, device, _ = plan.peer(d)
            part = self.whole.at[plan.core, index]
            self.copy(part, part, 2, d, device).wait_recv()
            if plan.pair == 2:
                self.back_copy(d, plan.core).start()

    def finish(self):
        plan = self.plan
        for d in plan.ways:
            self.gather_copy(d).wait_send()
        if plan.pair == 2:
            for d in range(len(plan.ways) + 1):
                self.back_copy(d, plan.core).wait_send()
                self.back_copy(d, 1 - plan.core).wait_recv()


def slabs(sizes, chips):
    out, at = [], 0
    for size in sizes:
        chunk = up_to(-(-size // chips), 8)
        out.append((at, chunk))
        at += chunk
    return out


def slab_rows(sizes, chips):
    return sum(chunk for _, chunk in slabs(sizes, chips))


def summer_scratch(plan, sizes):
    rows, dma, n = slab_rows(sizes, plan.chips), pltpu.SemaphoreType.DMA, max(len(plan.ways), 1)
    full = (plan.chips, rows, plan.lanes)
    return [pltpu.VMEM((plan.pair,) + full, F32), pltpu.VMEM((plan.pair,) + full, BF), pltpu.VMEM(full, BF),
            pltpu.VMEM(full, BF), pltpu.VMEM((n, rows, plan.lanes), BF),
            dma((1,)), dma((1,)), dma((n,)), dma((n,)), dma((n,)), dma((n,)), dma((n + 1,)), dma((n + 1,))]


SUMMER_REFS = 13
LATE_AT = 1
UNITS, SIDE = 2, 256


NAMES = ("local", "halo", "features", "halo_first", "halo_second", "halo_third", "return_second", "return_third",
         "weight_first", "weight_second", "weight_third", "index_row", "labels")


def product(accs, lhs, rhs, depth, transpose=False):
    for k in depth:
        for q in range(UNITS):
            pltpu.matmul_push_rhs(rhs(k), staging_register=0, mxu_index=q, transpose=transpose)
            for i, acc in enumerate(accs[q]):
                pltpu.matmul_acc_lhs(acc, lhs(q, i, k), load_staged_rhs=0 if i == 0 else None)


def padded(value, rows, lanes=None):
    if value.shape[0] < rows:
        value = jnp.concatenate([value, jnp.zeros((rows - value.shape[0], value.shape[1]), value.dtype)], axis=0)
    if lanes is not None and value.shape[1] < lanes:
        value = jnp.concatenate([value, jnp.zeros((value.shape[0], lanes - value.shape[1]), value.dtype)], axis=1)
    return value


def span(k):
    return slice(k * SIDE, (k + 1) * SIDE)


def step_kernel(plan, tiles, early_sizes, late_sizes, *refs):
    count = len(NAMES)
    hbm = dict(zip(NAMES, refs[:count]))
    whole_early, whole_late, n2, n3, b2, b3 = refs[count:count + 6]
    (in_sem, local_i, halo_i, x_t, values_two, values_three, scaled_three, scaled_two, w1, w2, w3, index_row, labels,
     near_far, back, halo_t, hits_t, inverse, mixed_t, mixed_two, mixed_two_t, mixed_three, slope_one, slope_two, upstream,
     upstream_three_t, target_held, w3_wide, s2, s3, o2, o3, hsend, hrecv, *relay) = refs[count + 6:count + 43]
    rest = refs[count + 43:]
    early, late = (Summer(plan, sizes, *part[:5], whole, part[5:]) for sizes, part, whole in (
        (early_sizes, rest[:SUMMER_REFS], whole_early), (late_sizes, rest[SUMMER_REFS:], whole_late)))
    nodes, slots = local_i.shape[0], halo_i.shape[1]
    every, width, classes = nodes + slots, x_t.shape[0], w3.shape[0]
    plan.place()

    own, other = pl.ds(0, nodes), pl.ds(nodes, slots)
    tall = nodes // tiles
    tile = [slice(t * tall, (t + 1) * tall) for t in range(tiles)]
    targets = {"features": (x_t, 1, 0), "halo_first": (x_t, 1, nodes), "halo_second": (values_two, 0, nodes),
               "halo_third": (values_three, 0, nodes), "return_second": (scaled_two, 0, nodes),
               "return_third": (scaled_three, 0, nodes), "weight_first": (w1, 0, 0), "weight_second": (w2, 0, 0),
               "weight_third": (w3, 0, 0), "index_row": (index_row, 0, 0), "labels": (labels, 0, 0)}
    slot = {}

    class Load:
        def __init__(self, key):
            self.key = key

        def copy(self):
            index = slot.setdefault(self.key, len(slot))
            if isinstance(self.key, tuple):
                name, t = self.key
                rows = pl.ds(t * tall, tall)
                return pltpu.make_async_copy(hbm[name].at[rows], {"local": local_i, "halo": halo_i}[name].at[rows], in_sem.at[index])
            ref, axis, start = targets[self.key]
            part = pl.ds(start, hbm[self.key].shape[axis])
            return pltpu.make_async_copy(hbm[self.key], ref.at[:, part] if axis else ref.at[part], in_sem.at[index])

        def start(self):
            self.copy().start()

        def wait(self):
            self.copy().wait()

    loads = {}

    def load(key):
        loads[key] = Load(key)
        loads[key].start()

    late_names = ("halo_second", "halo_third", "return_third", "return_second", "weight_third")

    def load_tile(t):
        load(("local", t))
        load(("halo", t))

    def load_named(names):
        for name in names:
            load(name)

    load_tile(0)
    first_names = ("features", "halo_first", "weight_first", "index_row", "labels", "weight_second")
    load_named(first_names)
    for t in range(1, tiles):
        load_tile(t)

    halo_clear(plan, (n2, n3, b2, b3))
    met = plan.greet()
    early.clear()
    late.clear()
    wide = target_held.shape[1]

    def mark():
        back[:, other] = jnp.where(lax.broadcasted_iota(jnp.int32, (nodes, slots), 0) == index_row[...], 1.0, 0.0).astype(BF)
        hits_t[...] = back[:, other].T
        target_held[...] = jnp.where(lax.broadcasted_iota(jnp.int32, (wide, nodes), 0) == labels[...], 1.0, 0.0).T
        w3_wide[...] = jnp.zeros_like(w3_wide)

    tail = up_to(width, 16 * UNITS) - UNITS * SIDE * (width // (UNITS * SIDE))
    body = width // (UNITS * SIDE)
    strip = tail // UNITS

    def first_rows(q, i):
        return ((q + UNITS * i) * SIDE, SIDE) if i < body else (UNITS * SIDE * body + q * strip, strip)

    def first_layer(*accs):
        mix = [[accs[q + UNITS * (i + (body + 1) * b)] for q in range(UNITS) for i in range(body + 1)] for b in range(2)]
        mix = [[m[q * (body + 1):(q + 1) * (body + 1)] for q in range(UNITS)] for m in mix]
        pres = accs[2 * UNITS * (body + 1):]
        for acc in accs:
            pltpu.matmul_pop(acc)

        def gather(t):
            loads[("local", t)].wait()
            loads[("halo", t)].wait()
            if t == LATE_AT:
                load_named(late_names)
            if t == tiles - 1:
                loads[late_names[0]].wait()
            near, far = local_i[tile[t], :].astype(F32), halo_i[tile[t], :].astype(F32)
            total = 1.0 + jnp.sum(near, axis=1, keepdims=True) + jnp.sum(far, axis=1, keepdims=True)
            near_far[tile[t], own] = near.astype(BF)
            near_far[tile[t], other] = far.astype(BF)
            square = near[:, tile[t]]
            here = lax.broadcasted_iota(jnp.int32, square.shape, 0) == lax.broadcasted_iota(jnp.int32, square.shape, 1)
            near_far[tile[t], tile[t]] = jnp.where(here, square + 1.0, square).astype(BF)
            inverse[tile[t], :] = jnp.broadcast_to(1.0 / total, (tall, inverse.shape[1]))

        def mix_tile(t):
            product(mix[t % 2], lambda q, i, k: padded(x_t[slice(first_rows(q, i)[0], min(sum(first_rows(q, i)), width)), span(k)], first_rows(q, i)[1]),
                    lambda k: near_far[tile[t], span(k)], range(every // SIDE), True)

        def settle(t):
            pre_acc = [pres[UNITS * (t % 2) + q] for q in range(UNITS)]
            half = tall // UNITS
            across = inverse[tile[t], :128].T[0:1]
            for i in range(body + 1):
                for q in range(UNITS):
                    start, size = first_rows(q, i)
                    mixed_t[start:start + size, tile[t]] = (pltpu.matmul_pop(mix[t % 2][q][i]) * across).astype(BF)
            back[own, tile[t]] = near_far[tile[t], own].T
            halo_t[:, tile[t]] = near_far[tile[t], other].T
            depth = -(-width // SIDE)
            turned = [mixed_t[k * SIDE:min((k + 1) * SIDE, mixed_t.shape[0]), tile[t]].T for k in range(depth)]
            product([[acc] for acc in pre_acc], lambda q, i, k: padded(turned[k][q * half:(q + 1) * half], half, SIDE),
                    lambda k: padded(w1[k * SIDE:min((k + 1) * SIDE, width), :], SIDE), range(depth))

        def close(t):
            half = tall // UNITS
            for q in range(UNITS):
                rows = slice(t * tall + q * half, t * tall + (q + 1) * half)
                pre = pltpu.matmul_pop(pres[UNITS * (t % 2) + q])
                sigma = jax.nn.sigmoid(pre)
                values_two[rows, :] = (pre * sigma).astype(BF)
                slope_one[rows, :] = slope(pre, sigma)

        for t in range(tiles):
            gather(t)
            if t == 0:
                for name in first_names:
                    loads[name].wait()
            mix_tile(t)
            if t == 0:
                mark()
            if t > 1:
                close(t - 2)
            if t > 0:
                settle(t - 1)
        if tiles > 1:
            close(tiles - 2)
        settle(tiles - 1)
        close(tiles - 1)

    def accs_of(sizes):
        return [pltpu.ACC(q)((size, SIDE), F32) for size in sizes for q in range(UNITS)]

    sizes = ([SIDE] * body + [strip]) * 2 + [tall // UNITS] * 2
    pl.run_scoped(first_layer, *accs_of(sizes))

    order = list(range(nodes // SIDE, every // SIDE)) + list(range(nodes // SIDE))

    def rest_of_step(*accs):
        held = [[accs[q + UNITS * i] for i in range(6)] for q in range(UNITS)]
        first, second = [p[0:2] for p in held], [p[2:3] for p in held]
        middle, small, small_late = ([p[i] for p in held] for i in (3, 4, 5))

        def at(q, i):
            return slice((q + UNITS * i) * SIDE, (q + UNITS * i + 1) * SIDE)

        def tall_product(sets, left, right, depth, transpose=False, pieces=2):
            for i in range(pieces):
                product([[sets[q][i]] for q in range(UNITS)], lambda q, _, k: left[at(q, i), span(k)],
                        lambda k: right(k), depth, transpose)

        def pops(sets, use, pieces=2):
            for i in range(pieces):
                for q in range(UNITS):
                    use(at(q, i), pltpu.matmul_pop(sets[q][i]))

        def keep_mixed(mixed, mixed_turned):
            def use(rows, value):
                out = (value * inverse[rows, :]).astype(BF)
                mixed[rows, :] = out
                if mixed_turned is not None:
                    mixed_turned[:, rows] = out.T
            return use

        def keep(out):
            def use(rows, value):
                out[rows, :] = value.astype(BF)
            return use

        def keep_scaled(out):
            def use(rows, value):
                out[rows, :] = (value * inverse[rows, :]).astype(BF)
            return use

        tall_product(first, near_far, lambda k: values_two[span(k), :], order)
        tall_product(second, hits_t, lambda k: values_two[span(k), :], range(nodes // SIDE), pieces=1)
        pops(first, keep_mixed(mixed_two, mixed_two_t))
        pops(second, keep(s2), pieces=1)
        for name in late_names[1:]:
            loads[name].wait()
        w3_wide[0:classes, :] = w3[...]
        met()
        halo_start(plan, s2, n2, hsend, hrecv, 0, relay)
        tall_product(first, mixed_two, lambda k: w2[...], range(1))

        def activate(rows, pre):
            sigma = jax.nn.sigmoid(pre)
            values_three[rows, :] = (pre * sigma).astype(BF)
            slope_two[rows, :] = slope(pre, sigma)

        pops(first, activate)
        tall_product(first, near_far, lambda k: values_three[span(k), :], order)
        tall_product(second, hits_t, lambda k: values_three[span(k), :], range(nodes // SIDE), pieces=1)
        pops(first, keep_mixed(mixed_three, None))
        tall_product(first, mixed_three, lambda k: w3_wide[...], range(1), True)
        pops(second, keep(s3), pieces=1)
        ups = {}

        def soften(rows, logits):
            logits = logits[:, :wide]
            inside = lax.broadcasted_iota(jnp.int32, logits.shape, 1) < classes
            expo = jnp.where(inside, jnp.exp(logits), 0.0)
            probs = expo / jnp.sum(expo, axis=1, keepdims=True)
            up = ((probs - target_held[rows, :]) / nodes).astype(BF)
            upstream_three_t[:, rows] = up.T
            ups[rows.start] = padded(up, up.shape[0], SIDE)

        pops(first, soften)
        for i in range(2):
            product([[first[q][i]] for q in range(UNITS)], lambda q, _, k: ups[at(q, i).start], lambda k: w3_wide[...], range(1))
        pops(first, keep_scaled(scaled_three))
        halo_start(plan, s3, n3, hsend, hrecv, 1, relay)
        tall_product(first, back, lambda k: scaled_three[span(k), :], order)
        stripes = nodes // SIDE // UNITS
        for k in range(stripes):
            for q in range(UNITS):
                pltpu.matmul_push_rhs(mixed_three[span(q * stripes + k), :], staging_register=0, mxu_index=q)
                pltpu.matmul_acc_lhs(small[q], upstream_three_t[0:small_rows, span(q * stripes + k)], load_staged_rhs=0)
        tall_product(second, halo_t, lambda k: scaled_three[span(k), :], range(nodes // SIDE), pieces=1)

        def climb(slopes):
            def use(rows, value):
                upstream[rows, :] = (value * slopes[rows, :]).astype(BF)
            return use

        pops(first, climb(slope_two))
        tall_product(first, upstream, lambda k: w2[...], range(1), True)
        early.put(1, pltpu.matmul_pop(small[0]) + pltpu.matmul_pop(small[1]))
        pops(second, keep(o3), pieces=1)
        half = mixed_two_t.shape[0] // UNITS
        for k in range(nodes // SIDE):
            for q in range(UNITS):
                pltpu.matmul_push_rhs(upstream[span(k), :], staging_register=0, mxu_index=q)
                pltpu.matmul_acc_lhs(middle[q], mixed_two_t[q * half:(q + 1) * half, span(k)], load_staged_rhs=0)
        pops(first, keep_scaled(scaled_two))
        for q in range(UNITS):
            early.put(0, pltpu.matmul_pop(middle[q]), q * half)
        early.start_pair()
        relay_start(plan, n2, hrecv, 0, relay)
        halo_start(plan, o3, b3, hsend, hrecv, 2)
        tall_product(first, back, lambda k: scaled_two[span(k), :], order)
        tall_product(second, halo_t, lambda k: scaled_two[span(k), :], range(nodes // SIDE), pieces=1)
        early.start_spread()
        pops(first, climb(slope_one))
        product([first[q][:body] + [small_late[q]] for q in range(UNITS)],
                lambda q, i, k: mixed_t[slice(first_rows(q, i)[0], sum(first_rows(q, i))), span(k)],
                lambda k: upstream[span(k), :], range(nodes // SIDE))
        pops(second, keep(o2), pieces=1)
        for i in range(body + 1):
            for q in range(UNITS):
                late.put(0, pltpu.matmul_pop((first[q][:body] + [small_late[q]])[i]), first_rows(q, i)[0])
        late.start_pair()

    small_rows = up_to(classes, 16)
    pl.run_scoped(rest_of_step, *accs_of([SIDE] * 3 + [mixed_two_t.shape[0] // UNITS, small_rows, strip]))
    late.start_spread()
    relay_start(plan, n3, hrecv, 1, relay)
    early.start_gather()
    late.start_gather()
    halo_start(plan, o2, b2, hsend, hrecv, 3)
    early.start_back()
    early.finish()
    late.start_back()
    late.finish()
    relay_finish(plan, n2, hrecv, 0, relay)
    relay_finish(plan, n3, hrecv, 1, relay)
    for way, (src, dst) in enumerate(((s2, n2), (s3, n3), (o3, b3), (o2, b2))):
        halo_finish(plan, src, dst, hsend, hrecv, way)


def finish_kernel(plan, early_sizes, late_sizes, whole_early, whole_late, n2, n3, b2, b3, g1, g2, g3, m2, m3, a2, a3, h1, h2, h3, sem):
    copies = [pltpu.make_async_copy(src, dst, sem.at[i]) for i, (src, dst) in enumerate(((n2, m2), (n3, m3), (b2, a2), (b3, a3)))]
    for copy in copies:
        copy.start()
    for i, (ref, out, whole, sizes, part) in enumerate((
            (h1, g1, whole_late, late_sizes, 0), (h2, g2, whole_early, early_sizes, 0), (h3, g3, whole_early, early_sizes, 1))):
        at, chunk = slabs(sizes, plan.chips)[part]
        for core in range(plan.pair):
            for k in range(-(-ref.shape[0] // chunk)):
                rows = min(chunk, ref.shape[0] - k * chunk)
                ref[k * chunk:k * chunk + rows, core * plan.lanes:(core + 1) * plan.lanes] = whole[core, k, at:at + rows, :].astype(F32)
        copies.append(pltpu.make_async_copy(ref, out, sem.at[4 + i]))
        copies[-1].start()
    for copy in copies:
        copy.wait()


def per_device(mesh, features, local_mask, halo_mask, boundary_index, labels, halo_first, halo_second, halo_third,
               return_second, return_third, weight_first, weight_second, weight_third):
    features, local_mask, halo_mask = features[0, 0], local_mask[0, 0], halo_mask[0, 0]
    index, labels = boundary_index[0, 0], labels[0, 0]
    halo_first, halo_second, halo_third = halo_first[0, 0], halo_second[0, 0], halo_third[0, 0]
    return_second, return_third = return_second[0, 0], return_third[0, 0]
    nodes, width = features.shape
    slots, hidden, classes = index.shape[0], weight_first.shape[1], weight_third.shape[1]
    plan = Plan(mesh, hidden)
    early_sizes, late_sizes = (weight_second.shape[0], classes), (width,)
    tiles = 4 if nodes % 512 == 0 else 1
    values = (local_mask, halo_mask, features.T, halo_first.T, halo_second, halo_third, return_second, return_third,
              weight_first, weight_second, weight_third.T, index[None, :], labels[None, :])
    values = tuple(pltpu.with_memory_space_constraint(v, pltpu.HBM) for v in values)
    vmem, anywhere = pl.BlockSpec(memory_space=pltpu.VMEM), pl.BlockSpec(memory_space=pl.ANY)
    dma = pltpu.SemaphoreType.DMA
    block = jax.ShapeDtypeStruct((slots, hidden), BF)
    every = nodes + slots

    def held(value):
        return pltpu.VMEM(value.shape, value.dtype)

    done = pl.pallas_call(
        functools.partial(step_kernel, plan, tiles, early_sizes, late_sizes),
        out_shape=tuple(jax.ShapeDtypeStruct((plan.pair, plan.chips, slab_rows(sizes, plan.chips), plan.lanes), BF)
                        for sizes in (early_sizes, late_sizes)) + (block,) * 4,
        in_specs=[anywhere] * len(values), out_specs=(vmem,) * 6,
        scratch_shapes=[
            dma((len(values) + 2 * tiles,)), held(local_mask), held(halo_mask), pltpu.VMEM((width, every), BF),
            pltpu.VMEM((every, hidden), BF), pltpu.VMEM((every, hidden), BF), pltpu.VMEM((every, hidden), BF),
            pltpu.VMEM((every, hidden), BF), held(values[8]), held(values[9]), held(values[10]), held(values[11]), held(values[12]),
            pltpu.VMEM((nodes, every), BF), pltpu.VMEM((nodes, every), BF), pltpu.VMEM((slots, nodes), BF),
            pltpu.VMEM((slots, nodes), BF), pltpu.VMEM((nodes, hidden), F32), pltpu.VMEM((up_to(width, 16 * UNITS), nodes), BF),
            pltpu.VMEM((nodes, hidden), BF), pltpu.VMEM((hidden, nodes), BF), pltpu.VMEM((nodes, hidden), BF), pltpu.VMEM((nodes, hidden), F32),
            pltpu.VMEM((nodes, hidden), F32), pltpu.VMEM((nodes, hidden), BF), pltpu.VMEM((up_to(classes, 128), nodes), BF),
            pltpu.VMEM((nodes, up_to(classes, 128)), F32), pltpu.VMEM((SIDE, hidden), BF)]
        + [pltpu.VMEM((slots, hidden), BF)] * 4 + [dma((4, 4)), dma((4, 4)), pltpu.VMEM((2, slots // 4, hidden), BF), dma((2,)), dma((2,))]
        + summer_scratch(plan, early_sizes) + summer_scratch(plan, late_sizes),
        compiler_params=pltpu.CompilerParams(collective_id=0, has_side_effects=True, vmem_limit_bytes=40 * 2**20),
        name="step",
    )(*values)
    grads = ((weight_first.shape, F32), (weight_second.shape, F32), (weight_third.shape[::-1], F32))
    out = pl.pallas_call(
        functools.partial(finish_kernel, plan, early_sizes, late_sizes),
        out_shape=tuple(jax.ShapeDtypeStruct(*g) for g in grads) + (block,) * 4,
        in_specs=[vmem] * 6, out_specs=(anywhere,) * 7,
        scratch_shapes=[pltpu.VMEM(*g) for g in grads] + [dma((7,))],
        compiler_params=pltpu.CompilerParams(vmem_limit_bytes=16 * 2**20), name="finish",
    )(*done)
    return (out[0], out[1], out[2].T) + tuple(v[None, None] for v in out[3:])


def solution(mesh):
    wide, flat, copied = P("row", "col", None, None), P("row", "col", None), P()
    return jax.shard_map(
        functools.partial(per_device, mesh), mesh=mesh,
        in_specs=(wide, wide, wide, flat, flat, wide, wide, wide, wide, wide, copied, copied, copied),
        out_specs=(copied, copied, copied, wide, wide, wide, wide),
        check_vma=False,
    )
```
